128 devices in a mesh: section: 16 (over z_lo, y, core), ep: 8 (over z_hi, x).
Axes of the slice: x: 4, y: 4, z: 4 (z_hi: 2, z_lo: 2; z = z_hi * 2 + z_lo), core: 2. Of those that a mesh axis runs over, the one named last changes fastest.
Arguments:
- fwd_input: bfloat16 [16, 1024, 3584], P('section', 'ep'), may hold values from -6 to 6
- bwd_input: bfloat16 [16, 1024, 3584], P('section', 'ep'), may hold values from -6 to 6
- bwd_grad: bfloat16 [16, 1024, 3584], P('section', 'ep'), may hold values from -6 to 6
- fwd_ids: int32 [16, 1024, 2], P('section', 'ep'), may hold values from 0 to 7, all different within a row; in each aligned block of 128 rows (0 to 127, 128 to 255, ...) at most 48 rows name the same one
- bwd_ids: int32 [16, 1024, 2], P('section', 'ep'), may hold values from 0 to 7, all different within a row; in each aligned block of 128 rows (0 to 127, 128 to 255, ...) at most 48 rows name the same one
- norm_gain: float32 [16, 3584], P('section'), may hold values from 0.5 to 1.5
- router: bfloat16 [16, 3584, 8], P('section'), may hold values from -0.09375 to 0.09375
- gate_w: bfloat16 [16, 8, 3584, 1024], P('section', 'ep'), may hold values from -0.09375 to 0.09375
- up_w: bfloat16 [16, 8, 3584, 1024], P('section', 'ep'), may hold values from -0.09375 to 0.09375
- down_w: bfloat16 [16, 8, 1024, 3584], P('section', 'ep'), may hold values from -0.1875 to 0.1875
Outputs:
- fwd_next: bfloat16 [16, 1024, 3584], P('section', 'ep')
- bwd_prev: bfloat16 [16, 1024, 3584], P('section', 'ep')
The draws below stay inside these ranges and needn't reach their ends.
Inputs may be any that keep to these rules, and one draw needn't show every extreme that they name: `fwd_ids`: each token names 2 different experts of 0 to 7; among the 128 tokens of one index of ep in one section no expert is named more than 48 times, a bound that some block reaches. `bwd_ids`: each token names 2 different experts of 0 to 7; among the 128 tokens of one index of ep in one section no expert is named more than 48 times, a bound that some block reaches.
All inputs are finite; a program needn't handle non-finite values.
Results may differ from the reference program's by a relative error of at most 0.0035.
Values may be sent and summed in bfloat16 or wider, within the bound.
No kernel may reach another device: no remote copies, remote signals or barrier semaphores. Data moves between devices by JAX's collectives and lax.ppermute only.
A program may use at most 128 MiB of HBM per device.

```python
import math
import jax
import jax.numpy as jnp
import numpy as np
from jax import lax

D = 3584
F = 1024
TOP = 2
TOK_DEV = 128
SECTIONS = 16
EXPERTS = 8
TOKENS = 1024
CAP = 48
N_EP = 8


def block_scale(stream_key, dims, shards, smallest, largest):
    level = 1.0
    for dim, parts in shards:
        heights = jax.random.uniform(jax.random.fold_in(jax.random.fold_in(stream_key, 6), dim), (parts,), jnp.float32, smallest / len(shards), largest / len(shards))
        level = level * jnp.repeat(jnp.exp(heights), dims[dim] // parts).reshape((-1,) + (1,) * (len(dims) - 1 - dim))
    return level


def deal_out(rng, own, number, rows, amount, top, limit, lean):
    ranking = jax.random.permutation(rng, amount)
    crowded, usual = portions_of(amount, rows * top, limit, lean, True), portions_of(amount, rows * top, limit, lean, False)
    places = jnp.arange(amount)

    def named(tallies, offset_by):
        used = int((tallies > 0).sum())
        fixed = max(1, used // 4)
        shifted = fixed + (places - fixed + offset_by * (used - fixed)) % max(1, amount - fixed)
        return jnp.zeros((amount,), jnp.int32).at[ranking[jnp.where(places < fixed, places, shifted)]].set(jnp.asarray(tallies, jnp.int32))

    tallies = jnp.where(number % 4 == 0, named(crowded, number // 4), named(usual, number - number // 4 - 1))
    mixed = jax.random.permutation(jax.random.fold_in(own, 3), amount)
    source_of, taker = mixed[0:amount // 2 * 2:2], mixed[1:amount // 2 * 2:2]
    slack = jnp.minimum(tallies[source_of] - 1, limit - tallies[taker]) // 2
    slack = jnp.where((source_of == ranking[0]) | (taker == ranking[0]) | (tallies[taker] == 0), 0, jnp.maximum(slack, 0))
    shifted = jax.random.randint(jax.random.fold_in(own, 4), (amount // 2,), 0, 1 << 20) % (slack + 1)
    tallies = tallies.at[source_of].add(-shifted).at[taker].add(shifted)
    items = jnp.searchsorted(jnp.cumsum(tallies), jnp.arange(rows * top), side="right").astype(jnp.int32)
    grid = items.reshape(top, rows).T
    grid = grid[jax.random.permutation(jax.random.fold_in(own, 1), rows)]
    offset_by = jax.random.randint(jax.random.fold_in(own, 2), (rows, 1), 0, top)
    return jnp.take_along_axis(grid, (jnp.arange(top)[None, :] + offset_by) % top, axis=1)


def portions_of(count, total, limit, slope, full):
    portions = [(1 << 20) // math.isqrt(standing ** slope) + 1 for standing in range(1, count + 1)]
    largest = limit if full else min(limit, max(-(-total // count), total * portions[0] // sum(portions)))
    least = 1 if total - largest >= count - 1 else 0
    counts, surplus = [largest] + [least] * (count - 1), total - largest - least * (count - 1)
    while surplus > 0:
        candidates = [i for i in range(1, count) if counts[i] < largest] or [i for i in range(1, count) if counts[i] < limit]
        whole, left = sum([portions[i] for i in candidates]), surplus
        for i in candidates:
            extra = min(limit - counts[i], max(1, left * portions[i] // whole), surplus)
            counts[i] = counts[i] + extra
            surplus = surplus - extra
    return np.array(counts)


def bell_draw(key, shape, deviation, limit, split=(), kind=jnp.bfloat16):
    gain = block_scale(key, shape, split, -0.22, 0.18) if split else 1.0
    values = jax.random.normal(key, shape, jnp.float32) * deviation * gain
    return jnp.minimum(jnp.maximum(values, -limit), limit).astype(kind)


def setup_inputs(seed: int = 0) -> dict:
    seeds = jax.random.split(jax.random.key(seed), 11)
    fwd_input = bell_draw(seeds[0], (SECTIONS, TOKENS, D), 1.0, 6.0, ((0, 16), (1, 8)))
    bwd_input = bell_draw(seeds[1], (SECTIONS, TOKENS, D), 1.0, 6.0, ((0, 16), (1, 8)))
    bwd_grad = bell_draw(seeds[2], (SECTIONS, TOKENS, D), 1.0, 6.0, ((0, 16), (1, 8)))
    fwd_ids_keys = jax.random.split(jax.random.fold_in(seeds[3], 1), SECTIONS * TOKENS // TOK_DEV)
    fwd_ids_turns = jax.random.permutation(jax.random.fold_in(seeds[3], 3), SECTIONS * TOKENS // TOK_DEV)
    fwd_ids = jax.vmap(lambda own, number: deal_out(jax.random.fold_in(seeds[3], 2), own, number, TOK_DEV, EXPERTS, TOP, CAP, 1))(fwd_ids_keys, fwd_ids_turns).reshape((SECTIONS, TOKENS, TOP))
    bwd_ids_keys = jax.random.split(jax.random.fold_in(seeds[4], 1), SECTIONS * TOKENS // TOK_DEV)
    bwd_ids_turns = jax.random.permutation(jax.random.fold_in(seeds[4], 3), SECTIONS * TOKENS // TOK_DEV)
    bwd_ids = jax.vmap(lambda own, number: deal_out(jax.random.fold_in(seeds[4], 2), own, number, TOK_DEV, EXPERTS, TOP, CAP, 1))(bwd_ids_keys, bwd_ids_turns).reshape((SECTIONS, TOKENS, TOP))
    norm_gain = jnp.clip(1.0 + 0.1 * jax.random.normal(seeds[5], (SECTIONS, D), jnp.float32), 0.5, 1.5)
    router = bell_draw(seeds[6], (SECTIONS, D, EXPERTS), D ** -0.5, 0.09375, ((0, 16),))
    gate_w = bell_draw(seeds[7], (SECTIONS, EXPERTS, D, F), D ** -0.5, 0.09375, ((0, 16), (1, 8)))
    up_w = bell_draw(seeds[8], (SECTIONS, EXPERTS, D, F), D ** -0.5, 0.09375, ((0, 16), (1, 8)))
    down_w = bell_draw(seeds[9], (SECTIONS, EXPERTS, F, D), F ** -0.5, 0.1875, ((0, 16), (1, 8)))
    return {"fwd_input": fwd_input, "bwd_input": bwd_input, "bwd_grad": bwd_grad, "fwd_ids": fwd_ids, "bwd_ids": bwd_ids, "norm_gain": norm_gain, "router": router, "gate_w": gate_w, "up_w": up_w, "down_w": down_w}


NORM_EPSILON = 1e-06
ROUTE_SCALE = 2.5

def norm_rows(hidden, gain_vec):
    hidden_f32 = hidden.astype(jnp.float32)
    inverse = lax.rsqrt(lax.optimization_barrier(jnp.mean(hidden_f32 * hidden_f32, axis=1, keepdims=True)) + NORM_EPSILON)
    return ((hidden_f32 * inverse * gain_vec).astype(jnp.bfloat16), inverse)

def routing(normed, router_mat, expert_ids):
    logits = jnp.dot(normed, router_mat, preferred_element_type=jnp.float32)
    scores = jax.nn.sigmoid(logits)
    picked = jnp.take_along_axis(scores, expert_ids, axis=1)
    total_score = lax.optimization_barrier(jnp.sum(picked, axis=1, keepdims=True))
    return (scores, total_score, picked / total_score)

def slot_table(expert_ids, n_experts, slot_room):
    flat_ids = expert_ids.reshape(-1).astype(jnp.int32)
    entry_count = flat_ids.shape[0]
    sort_order = jnp.argsort(flat_ids, stable=True).astype(jnp.int32)
    expert_counts = jax.ops.segment_sum(jnp.ones((entry_count,), jnp.int32), flat_ids, num_segments=n_experts).astype(jnp.int32)
    group_starts = jnp.cumsum(expert_counts).astype(jnp.int32) - expert_counts
    ranks_sorted = jnp.arange(entry_count, dtype=jnp.int32) - group_starts[flat_ids[sort_order]]
    slot_ranks = jnp.zeros((entry_count,), jnp.int32).at[sort_order].set(ranks_sorted)
    slot_index = flat_ids * slot_room + slot_ranks
    slot_owner = jnp.full((n_experts * slot_room,), -1, jnp.int32).at[slot_index].set(jnp.arange(entry_count, dtype=jnp.int32))
    return (slot_index, slot_owner)

def pack_rows(row_data, slot_owner, row_stride):
    slot_valid = slot_owner >= 0
    source_row = jnp.where(slot_valid, slot_owner // row_stride, 0).astype(jnp.int32)
    return jnp.where(slot_valid[:, None], row_data[source_row], jnp.zeros((), row_data.dtype))

def section_step(inputs):
    fwd_h, bwd_h, grad_out, ids_fwd, ids_bwd, gain_vec, router_mat, gate_mats, up_mats, down_mats = inputs
    n_experts = router_mat.shape[1]
    slot_room = N_EP * CAP
    model_width = fwd_h.shape[1]
    token_count = fwd_h.shape[0]
    gate_f32 = gate_mats.astype(jnp.float32)
    up_f32 = up_mats.astype(jnp.float32)
    down_f32 = down_mats.astype(jnp.float32)

    def forward(hidden, expert_ids):
        normed, inverse = norm_rows(hidden, gain_vec)
        scores, total_score, weights = routing(normed, router_mat, expert_ids)
        slot_index, slot_owner = slot_table(expert_ids, n_experts, slot_room)
        expert_rows = pack_rows(normed, slot_owner, TOP).reshape(n_experts, slot_room, model_width)
        rows_f32 = expert_rows.astype(jnp.float32)
        gate_val = jnp.einsum('erd,edf->erf', rows_f32, gate_f32)
        up_val = jnp.einsum('erd,edf->erf', rows_f32, up_f32)
        active = (jax.nn.silu(gate_val) * up_val).astype(jnp.bfloat16)
        output = jnp.einsum('erf,efd->erd', active.astype(jnp.float32), down_f32).astype(jnp.bfloat16)
        picked_rows = output.reshape(-1, model_width)[slot_index].reshape(token_count, TOP, model_width)
        mixed = hidden.astype(jnp.float32) + ROUTE_SCALE * lax.optimization_barrier(jnp.sum(weights[:, :, None] * picked_rows.astype(jnp.float32), axis=1))
        return (mixed.astype(jnp.bfloat16), (normed, inverse, scores, total_score, weights, slot_index, slot_owner, gate_val, up_val, picked_rows))
    mixed_fwd, _ = forward(fwd_h, ids_fwd)
    _, saved = forward(bwd_h, ids_bwd)
    normed, inverse, scores, total_score, weights, slot_index, slot_owner, gate_val, up_val, picked_rows = saved
    grad_top = grad_out.astype(jnp.float32)
    d_weights = ROUTE_SCALE * lax.optimization_barrier(jnp.sum(grad_top[:, None, :] * picked_rows.astype(jnp.float32), axis=2))
    d_rows = (ROUTE_SCALE * weights[:, :, None] * grad_top[:, None, :]).astype(jnp.bfloat16)
    packed_grads = pack_rows(d_rows.reshape(token_count * TOP, model_width), slot_owner, 1)
    grads_f32 = packed_grads.reshape(n_experts, slot_room, model_width).astype(jnp.float32)
    d_active = jnp.einsum('erd,efd->erf', grads_f32, down_f32)
    gate_sigmoid = jax.nn.sigmoid(gate_val)
    d_gate = (d_active * up_val * gate_sigmoid * (1.0 + gate_val * (1.0 - gate_sigmoid))).astype(jnp.bfloat16)
    d_up = (d_active * gate_val * gate_sigmoid).astype(jnp.bfloat16)
    d_gate_f32 = d_gate.astype(jnp.float32)
    d_up_f32 = d_up.astype(jnp.float32)
    d_back = (jnp.einsum('erf,edf->erd', d_gate_f32, gate_f32) + jnp.einsum('erf,edf->erd', d_up_f32, up_f32)).astype(jnp.bfloat16)
    d_normed = lax.optimization_barrier(jnp.sum(d_back.reshape(-1, model_width)[slot_index].reshape(token_count, TOP, model_width).astype(jnp.float32), axis=1))
    d_picked = (d_weights - lax.optimization_barrier(jnp.sum(d_weights * weights, axis=1, keepdims=True))) / total_score
    token_index = jnp.arange(token_count, dtype=jnp.int32)[:, None]
    d_scores = jnp.zeros_like(scores).at[token_index, ids_bwd].add(d_picked)
    d_logits = (d_scores * scores * (1.0 - scores)).astype(jnp.bfloat16)
    d_normed = d_normed + jnp.dot(d_logits, router_mat.T, preferred_element_type=jnp.float32)
    hidden_f32 = bwd_h.astype(jnp.float32)
    scaled = gain_vec * d_normed
    d_hidden = inverse * scaled - hidden_f32 * inverse * inverse * inverse * lax.optimization_barrier(jnp.sum(scaled * hidden_f32, axis=1, keepdims=True)) / model_width
    d_input = (grad_top + d_hidden).astype(jnp.bfloat16)
    return (mixed_fwd, d_input)

def reference(fwd_input, bwd_input, bwd_grad, fwd_ids, bwd_ids, norm_gain, router, gate_w, up_w, down_w):
    mixed, d_input = lax.map(section_step, (fwd_input, bwd_input, bwd_grad, fwd_ids, bwd_ids, norm_gain, router, gate_w, up_w, down_w))
    fwd_next = jnp.roll(mixed, 1, axis=0)
    bwd_prev = jnp.roll(d_input, -1, axis=0)
    return (fwd_next, bwd_prev)
```

```python
import functools
import jax
import jax.numpy as jnp
from jax import lax
from jax.experimental import pallas as pl
from jax.experimental.pallas import tpu as pltpu
from jax.sharding import PartitionSpec as P


NORM_EPSILON = 1e-06
ROUTE_SCALE = 2.5

T = 128
D = 3584
F = 1024
CAP = 48
NX = 4
NZ = 2
ROWS = NX * NZ * CAP
TF = 256
TD = 512
EXT = 128
f32 = jnp.float32
bf16 = jnp.bfloat16
NT = (((1,), (1,)), ((), ()))


def call(body, outs, ins, grid=None, in_specs=None, out_specs=None, scratch=(), flops=0, after=None):
    kwargs = {}
    if after is not None:
        inner, count = body, len(ins)
        ins = (*ins, after)
        in_specs = [*in_specs, pl.BlockSpec(memory_space=pl.ANY)]

        def body(*refs):
            inner(*refs[:count], *refs[count + 1 :])

    if grid is not None:
        kwargs["grid"] = grid
    if in_specs is not None:
        kwargs["in_specs"] = in_specs
    if out_specs is not None:
        kwargs["out_specs"] = out_specs
    moved = sum(a.size * a.dtype.itemsize for a in ins) + sum(o.size * o.dtype.itemsize for o in outs)
    return pl.pallas_call(
        body,
        out_shape=outs,
        scratch_shapes=list(scratch),
        cost_estimate=pl.CostEstimate(flops=int(flops), bytes_accessed=int(moved), transcendentals=0),
        **kwargs,
    )(*ins)


def vspec(shape, index=None):
    fixed = index if index is not None else (0,) * len(shape)
    return pl.BlockSpec(shape, lambda *_: fixed)


def chip():
    return pl.BlockSpec(memory_space=pltpu.VMEM)


def sspec():
    return pl.BlockSpec(memory_space=pltpu.SMEM)


def shape(*dims, dtype=bf16):
    return jax.ShapeDtypeStruct(dims, dtype)


def slots_of(named, place_ref):
    half, column = place_ref[0], place_ref[1]
    lane = lax.broadcasted_iota(jnp.int32, (T, T), 1)
    row = lax.broadcasted_iota(jnp.int32, (T, T), 0)
    member = jnp.where((lane == named[0]) | (lane == named[1]), 1.0, 0.0).astype(bf16)
    before = jnp.where(lane < row, 1.0, 0.0).astype(bf16)
    rank = jnp.dot(before, member, preferred_element_type=f32)
    slots = []
    for name in named:
        own_rank = jnp.sum(jnp.where(lane == name, rank, 0.0), axis=1, keepdims=True)
        step = ((name - column) & (NX - 1)).astype(f32)
        slots.append(jnp.where((name >> 2) == half, step * CAP + own_rank, -1.0))
    return slots


def names_of(ids_ref, first):
    return [ids_ref[:, first + k : first + k + 1] for k in range(2)]


def pack(slots, row_tile, outs, weights=None):
    lane = lax.broadcasted_iota(jnp.int32, (T, 256), 1).astype(f32)
    hits = [lane == slot for slot in slots]
    chosen = jnp.transpose(jnp.where(hits[0] | hits[1], 1.0, 0.0))[: NX * CAP].astype(bf16)
    if weights is not None:
        scale = jnp.where(hits[0], weights[0], 0.0) + jnp.where(hits[1], weights[1], 0.0)
        scale = ROUTE_SCALE * jnp.sum(jnp.transpose(scale), axis=1, keepdims=True)[: NX * CAP]
    for n in range(D // TD):
        cols = slice(n * TD, (n + 1) * TD)
        picked = jnp.dot(chosen, row_tile(cols), preferred_element_type=f32)
        if weights is not None:
            picked = scale * picked
        picked = picked.astype(bf16)
        for step in range(NX):
            outs[step][:, cols] = picked[step * CAP : (step + 1) * CAP]


def prep_grad_body(aux_ref, rows_ref, *outs):
    aux = aux_ref[...]
    pack([aux[:, 0:1], aux[:, 1:2]], lambda cols: rows_ref[:, cols], outs, [aux[:, 2:3], aux[:, 3:4]])


def prep_norm_body(first, place_ref, ids_ref, rows_ref, gain_ref, router_ref, *refs):
    outs, aux_ref, normed_ref = refs[:NX], refs[NX], refs[NX + 1]
    named = names_of(ids_ref, first)
    slots = slots_of(named, place_ref)
    total = jnp.zeros((T, 1), f32)
    for n in range(D // TD):
        tile = rows_ref[:, n * TD : (n + 1) * TD].astype(f32)
        total = total + jnp.sum(tile * tile, axis=1, keepdims=True)
    inverse = lax.rsqrt(total / D + NORM_EPSILON)
    for n in range(D // TD):
        cols = slice(n * TD, (n + 1) * TD)
        normed_ref[:, cols] = (rows_ref[:, cols].astype(f32) * inverse * gain_ref[:, cols]).astype(bf16)
    pack(slots, lambda cols: normed_ref[:, cols], outs)
    logits = lax.dot_general(normed_ref[...], router_ref[...], NT, preferred_element_type=f32)
    scores = jax.nn.sigmoid(logits)
    lane = lax.broadcasted_iota(jnp.int32, scores.shape, 1)
    picked = [jnp.sum(jnp.where(lane == name, scores, 0.0), axis=1, keepdims=True) for name in named]
    both = picked[0] + picked[1]
    columns = slots + [p / both for p in picked] + picked + [both, inverse] + [name.astype(f32) for name in named]
    lane = lax.broadcasted_iota(jnp.int32, (T, 128), 1)
    aux = jnp.zeros((T, 128), f32)
    for i, column in enumerate(columns):
        aux = jnp.where(lane == i, column, aux)
    aux_ref[...] = aux


def gather_rows(pieces, rows_ref):
    for step in range(NX):
        for z in range(NZ):
            at = (step * NZ + z) * CAP
            rows_ref[at : at + CAP, :] = pieces[z * NX + step][...]


def lift_body(*refs):
    pieces, gate_ref, up_ref, a_ref, b_ref, rows_ref = refs[:8], refs[8], refs[9], refs[10], refs[11], refs[12]

    @pl.when(pl.program_id(0) == 0)
    def _():
        gather_rows(pieces, rows_ref)

    rows = rows_ref[...]
    a_ref[...] = jnp.dot(rows, gate_ref[...], preferred_element_type=f32)
    b_ref[...] = jnp.dot(rows, up_ref[...], preferred_element_type=f32)


def hidden_grad_body(*refs):
    pieces, down_ref, a_ref, b_ref = refs[:8], refs[8], refs[9], refs[10]
    d_gate_ref, d_up_ref, dot_ref, rows_ref = refs[11:]

    @pl.when(pl.program_id(0) == 0)
    def _():
        gather_rows(pieces, rows_ref)
        dot_ref[...] = jnp.zeros_like(dot_ref)

    d_act = lax.dot_general(rows_ref[...], down_ref[...], NT, preferred_element_type=f32)
    a, b = a_ref[...], b_ref[...]
    s = jax.nn.sigmoid(a)
    active = (a * s * b).astype(bf16).astype(f32)
    both = active * d_act
    dot_ref[...] += both[:, :128] + both[:, 128:]
    d_gate_ref[...] = (d_act * b * s * (1.0 + a * (1.0 - s))).astype(bf16)
    d_up_ref[...] = (d_act * a * s).astype(bf16)


def back_body(d_gate_ref, d_up_ref, dot_ref, gate_ref, up_ref, *outs):
    i = pl.program_id(0)
    back = lax.dot_general(d_gate_ref[...], gate_ref[...], NT, preferred_element_type=f32)
    back = back + lax.dot_general(d_up_ref[...], up_ref[...], NT, preferred_element_type=f32)
    back = back.astype(bf16)
    for step in range(NX):
        outs[step][:, pl.ds(pl.multiple_of(i * TD, TD), TD)] = back[step * NZ * CAP : (step + 1) * NZ * CAP]

    @pl.when(i == 0)
    def _():
        dots = jnp.sum(dot_ref[...], axis=1, keepdims=True)
        high = dots.astype(bf16).astype(f32)
        lane = lax.broadcasted_iota(jnp.int32, (ROWS, EXT), 1)
        extra = jnp.where(lane == 0, high, jnp.where(lane == 1, dots - high, 0.0)).astype(bf16)
        for step in range(NX):
            outs[step][:, D:] = extra[step * NZ * CAP : (step + 1) * NZ * CAP]


def hidden_body(*refs):
    pieces, gate_ref, up_ref, out_ref, rows_ref = refs[:8], refs[8], refs[9], refs[10], refs[11]

    @pl.when(pl.program_id(0) == 0)
    def _():
        gather_rows(pieces, rows_ref)

    rows = rows_ref[...]
    a = jnp.dot(rows, gate_ref[...], preferred_element_type=f32)
    b = jnp.dot(rows, up_ref[...], preferred_element_type=f32)
    out_ref[...] = (a * jax.nn.sigmoid(a) * b).astype(bf16)


def down_body(active_ref, down_ref, *outs):
    i = pl.program_id(0)
    out = jnp.dot(active_ref[...], down_ref[...], preferred_element_type=f32).astype(bf16)
    for z in range(NZ):
        for step in range(NX):
            at = (step * NZ + z) * CAP
            outs[z * NX + step][:, pl.ds(pl.multiple_of(i * TD, TD), TD)] = out[at : at + CAP]


def split_weights(values):
    high = values.astype(bf16)
    return high, (values - high.astype(f32)).astype(bf16)


def hits_of(aux):
    lane = lax.broadcasted_iota(jnp.int32, (T, 256), 1).astype(f32)
    return [lane == aux[:, k : k + 1] for k in range(2)]


def stack_pieces(pieces, rows_ref):
    for step in range(NX):
        rows_ref[step * CAP : (step + 1) * CAP, :] = pieces[step][...]
    rows_ref[NX * CAP :, :] = jnp.zeros((256 - NX * CAP, rows_ref.shape[1]), bf16)


def mix_body(with_input, aux_ref, *refs):
    pieces, base_ref, out_ref, rows_ref = refs[:NX], refs[NX], refs[NX + 1], refs[NX + 2]
    stack_pieces(pieces, rows_ref)
    aux = aux_ref[...]
    hits = hits_of(aux)
    weights = jnp.where(hits[0], aux[:, 2:3], 0.0) + jnp.where(hits[1], aux[:, 3:4], 0.0)
    high, low = split_weights(ROUTE_SCALE * weights)
    for n in range(D // TD):
        cols = slice(n * TD, (n + 1) * TD)
        rows = rows_ref[:, cols]
        total = jnp.dot(high, rows, preferred_element_type=f32) + jnp.dot(low, rows, preferred_element_type=f32)
        if with_input:
            total = total + base_ref[:, cols].astype(f32)
        out_ref[:, cols] = total.astype(bf16)


def grad_input_body(with_input, aux_ref, hidden_ref, gain_ref, router_ref, *refs):
    pieces, base_ref, out_ref, rows_ref, scaled_ref = refs[:NX], refs[NX], refs[NX + 1], refs[NX + 2], refs[NX + 3]
    stack_pieces(pieces, rows_ref)
    aux = aux_ref[...]
    hits = [jnp.where(hit, 1.0, 0.0) for hit in hits_of(aux)]
    named = (hits[0] + hits[1]).astype(bf16)
    extra = rows_ref[:, D:]
    pulls = []
    for hit in hits:
        found = jnp.dot(hit.astype(bf16), extra, preferred_element_type=f32)
        pulls.append(found[:, 0:1] + found[:, 1:2])
    inverse = aux[:, 7:8]
    lane = lax.broadcasted_iota(jnp.int32, (T, router_ref.shape[0]), 1).astype(f32)
    d_logits = jnp.zeros(lane.shape, f32)
    for k in range(2):
        weight, score = aux[:, 2 + k : 3 + k], aux[:, 4 + k : 5 + k]
        term = (pulls[k] - weight * (pulls[0] + pulls[1])) * (1.0 - score)
        d_logits = d_logits + jnp.where(lane == aux[:, 8 + k : 9 + k], term, 0.0)
    log_high, log_low = split_weights(d_logits)
    against = jnp.zeros((T, 1), f32)
    for n in range(D // TD):
        cols = slice(n * TD, (n + 1) * TD)
        rows = rows_ref[:, cols]
        route = router_ref[:, cols]
        total = jnp.dot(named, rows, preferred_element_type=f32)
        total = total + jnp.dot(log_high, route, preferred_element_type=f32)
        total = total + jnp.dot(log_low, route, preferred_element_type=f32)
        scaled = total * gain_ref[:, cols]
        scaled_ref[:, cols] = scaled
        against = against + jnp.sum(scaled * hidden_ref[:, cols].astype(f32), axis=1, keepdims=True)
    pull = inverse * inverse * inverse * against / D
    for n in range(D // TD):
        cols = slice(n * TD, (n + 1) * TD)
        out = inverse * scaled_ref[:, cols] - hidden_ref[:, cols].astype(f32) * pull
        if with_input:
            out = out + base_ref[:, cols].astype(f32)
        out_ref[:, cols] = out.astype(bf16)


def ep_route(dz, dx):
    route = []
    for i in range(NZ * NX):
        z, x = divmod(i, NX)
        route.append((i, ((z + dz) % NZ) * NX + (x + dx) % NX))
    return route


def relay_route(sections, ds, dz):
    route = []
    for s in range(sections):
        for i in range(NZ * NX):
            z, x = divmod(i, NX)
            route.append((s * NZ * NX + i, ((s + ds) % sections) * NZ * NX + ((z + dz) % NZ) * NX + x))
    return route


def across(block):
    return lax.ppermute(block, "ep", ep_route(1, 0))


def spread(pieces):
    moved = list(pieces)
    for dx in (1, 3, 2):
        moved[dx] = lax.ppermute(pieces[dx], "ep", ep_route(0, dx))
    return moved


def collect(pieces):
    moved = list(pieces)
    for dx in (1, 3, 2):
        moved[dx] = lax.ppermute(pieces[dx], "ep", ep_route(0, -dx))
    return moved


def relay(block, ds, dz):
    return lax.ppermute(block, ("section", "ep"), relay_route(lax.axis_size("section"), ds, dz))


def step(
    fwd_input, bwd_input, bwd_grad, fwd_ids, bwd_ids, norm_gain, router, gate_w, up_w, down_w
):
    h_f, h_b, g = fwd_input[0], bwd_input[0], bwd_grad[0]
    gate, up, down = gate_w[0, 0], up_w[0, 0], down_w[0, 0]
    router_t = jnp.pad(router[0].T, ((0, 8), (0, 0)))
    own_ids = jnp.concatenate([bwd_ids[0], fwd_ids[0]], axis=1)
    index = lax.axis_index("ep")
    place = jnp.stack([index // NX, index % NX]).astype(jnp.int32)

    far_ids = across(own_ids)
    far_b = across(h_b)
    far_g = across(g)
    far_f = across(h_f)

    packed = [shape(CAP, D)] * NX
    aux_shape = shape(T, 128, dtype=f32)
    full = vspec((T, D))
    aux_spec = chip()
    piece_specs = [chip()] * NX
    pack_flops = 2 * NX * CAP * T * D

    def prep_grad(where, rows, aux):
        return call(
            prep_grad_body, packed, (aux, rows), grid=(1,), in_specs=[aux_spec, chip() if where == "far" else full], out_specs=piece_specs,
            flops=pack_flops,
        )

    def prep_norm(where, rows, ids, first, after=None):
        outs = call(
            functools.partial(prep_norm_body, first), packed + [aux_shape],
            (place, ids, rows, norm_gain, router_t), grid=(1,),
            in_specs=[sspec(), chip(), chip() if "far" in where else full, vspec((1, D)), vspec((16, D))],
            out_specs=piece_specs + [aux_spec], scratch=[pltpu.VMEM((T, D), bf16)],
            flops=pack_flops, after=after,
        )
        return outs[:NX], outs[NX]

    packed_b, aux_b = prep_norm("b_own", h_b, own_ids, 0)
    b_own = spread(packed_b)
    packed_g = prep_grad("own", g, aux_b)
    g_own = spread(packed_g)
    packed_bf, aux_b_far = prep_norm("b_far", far_b, far_ids, 0, packed_g[0])
    b_far = spread(packed_bf)
    packed_gf = prep_grad("far", far_g, aux_b_far)
    g_far = spread(packed_gf)
    packed_f, aux_f = prep_norm("f_own", h_f, own_ids, 2, packed_gf[0])
    f_own = spread(packed_f)

    eight = [chip()] * 8
    rows_scratch = pltpu.VMEM((ROWS, D), bf16)
    wide = pl.BlockSpec((D, TF), lambda i: (0, i))
    hidden_spec = pl.BlockSpec((ROWS, TF), lambda i: (0, i))
    dots_spec = vspec((ROWS, 128))
    hidden_f32 = shape(ROWS, F, dtype=f32)
    mat_flops = 2 * ROWS * D * F

    a, b = call(
        lift_body, [hidden_f32] * 2, (*b_own, *b_far, gate, up), grid=(F // TF,),
        in_specs=eight + [wide, wide], out_specs=[hidden_spec] * 2, scratch=[rows_scratch],
        flops=2 * mat_flops, after=packed_f[0],
    )
    packed_ff, aux_f_far = prep_norm("f_far", far_f, far_ids, 2, a)
    f_far = spread(packed_ff)
    d_gate, d_up, dots = call(
        hidden_grad_body, [shape(ROWS, F), shape(ROWS, F), shape(ROWS, 128, dtype=f32)],
        (*g_own, *g_far, down, a, b), grid=(F // TF,),
        in_specs=eight + [pl.BlockSpec((TF, D), lambda i: (i, 0)), hidden_spec, hidden_spec],
        out_specs=[hidden_spec, hidden_spec, dots_spec], scratch=[rows_scratch], flops=mat_flops,
        after=packed_ff[0],
    )
    tall = pl.BlockSpec((TD, F), lambda i: (i, 0))
    returned = call(
        back_body, [shape(NZ * CAP, D + EXT)] * NX, (d_gate, d_up, dots, gate, up), grid=(D // TD,),
        in_specs=[vspec((ROWS, F)), vspec((ROWS, F)), dots_spec, tall, tall],
        out_specs=[chip()] * NX, flops=2 * mat_flops,
    )
    back = collect(returned)

    (active,) = call(
        hidden_body, [shape(ROWS, F)], (*f_own, *f_far, gate, up), grid=(F // TF,),
        in_specs=eight + [wide, wide], out_specs=[hidden_spec], scratch=[rows_scratch],
        flops=2 * mat_flops, after=returned[0],
    )
    outputs = call(
        down_body, [shape(CAP, D)] * 8, (active, down), grid=(D // TD,),
        in_specs=[vspec((ROWS, F)), pl.BlockSpec((F, TD), lambda i: (0, i))], out_specs=eight,
        flops=mat_flops,
    )
    y_far = collect(outputs[NX:])
    y_own = collect(outputs[:NX])

    def mix(pieces, aux, base, with_input, after):
        return call(
            functools.partial(mix_body, with_input), [shape(T, D)], (aux, *pieces, base), grid=(1,),
            in_specs=[aux_spec] + piece_specs + [full if with_input else vspec((16, D))],
            out_specs=[full], scratch=[pltpu.VMEM((256, D), bf16)], flops=2 * pack_flops, after=after,
        )[0]

    def grad_input(z, aux, hidden, base, with_input, after):
        halves = [vspec((CAP, D + EXT), (z, 0))] * NX
        return call(
            functools.partial(grad_input_body, with_input), [shape(T, D)],
            (aux, hidden, norm_gain, router_t, *back, base), grid=(1,),
            in_specs=[aux_spec, full, vspec((1, D)), vspec((16, D))] + halves
            + [full if with_input else vspec((16, D))],
            out_specs=[full], scratch=[pltpu.VMEM((256, D + EXT), bf16), pltpu.VMEM((T, D), f32)],
            flops=2 * pack_flops, after=after,
        )[0]

    part_far = grad_input(1, aux_b_far, far_b, far_b, False, outputs[0])
    prev_far = relay(part_far, -1, 1)
    part_own = grad_input(0, aux_b, h_b, g, True, part_far)
    prev_own = relay(part_own, -1, 0)
    mix_far = mix(y_far, aux_f_far, far_f, False, part_own)
    next_far = relay(mix_far, 1, 1)
    mix_own = mix(y_own, aux_f, h_f, True, mix_far)
    next_own = relay(mix_own, 1, 0)

    def join(a, b):
        return (a.astype(f32) + b.astype(f32)).astype(bf16)

    return (join(next_own, next_far)[None], join(prev_own, prev_far)[None])


def solution(mesh):
    placed = (
        P("section", "ep", None),
        P("section", "ep", None),
        P("section", "ep", None),
        P("section", "ep", None),
        P("section", "ep", None),
        P("section", None),
        P("section", None, None),
        P("section", "ep", None, None),
        P("section", "ep", None, None),
        P("section", "ep", None, None),
    )
    return jax.shard_map(
        step,
        mesh=mesh,
        in_specs=placed,
        out_specs=(P("section", "ep", None), P("section", "ep", None)),
        check_vma=False,
    )
```

```python
import functools
import jax
import jax.numpy as jnp
from jax import lax
from jax.experimental import pallas as pl
from jax.experimental.pallas import tpu as pltpu
from jax.sharding import PartitionSpec as P


NORM_EPSILON = 1e-06
ROUTE_SCALE = 2.5

T = 128
D = 3584
F = 1024
CAP = 48
NX = 4
NZ = 2
EXPERTS = NX * NZ
ROWS = NX * NZ * CAP
TF = 512
TB = 1792
TD = 512
EXT = 128
f32 = jnp.float32
bf16 = jnp.bfloat16
NT = (((1,), (1,)), ((), ()))


def call(body, outs, ins, grid=None, in_specs=None, out_specs=None, scratch=(), flops=0, after=None):
    kwargs = {}
    if after is not None:
        inner, count = body, len(ins)
        ins = (*ins, after)
        in_specs = [*in_specs, pl.BlockSpec(memory_space=pl.ANY)]

        def body(*refs):
            inner(*refs[:count], *refs[count + 1 :])

    if grid is not None:
        kwargs["grid"] = grid
    if in_specs is not None:
        kwargs["in_specs"] = in_specs
    if out_specs is not None:
        kwargs["out_specs"] = out_specs
    moved = sum(a.size * a.dtype.itemsize for a in ins) + sum(o.size * o.dtype.itemsize for o in outs)
    return pl.pallas_call(
        body,
        out_shape=outs,
        scratch_shapes=list(scratch),
        cost_estimate=pl.CostEstimate(flops=int(flops), bytes_accessed=int(moved), transcendentals=0),
        **kwargs,
    )(*ins)


def vspec(shape, index=None):
    fixed = index if index is not None else (0,) * len(shape)
    return pl.BlockSpec(shape, lambda *_: fixed)


def chip():
    return pl.BlockSpec(memory_space=pltpu.VMEM)


def sspec():
    return pl.BlockSpec(memory_space=pltpu.SMEM)


def shape(*dims, dtype=bf16):
    return jax.ShapeDtypeStruct(dims, dtype)


def each_tile(body, start=0):
    carry = start
    for n in range(D // TD):
        carry = body(slice(n * TD, (n + 1) * TD), carry)
    return carry


def rows_iota(count):
    return lax.broadcasted_iota(jnp.int32, (count, T), 0)


def slots_of(named, place_ref):
    half, column = place_ref[0] >> 2, place_ref[0] & (NX - 1)
    expert = rows_iota(16)
    member = jnp.where((expert == named[0]) | (expert == named[1]), 1.0, 0.0).astype(bf16)
    before = jnp.where(rows_iota(T) < lax.broadcasted_iota(jnp.int32, (T, T), 1), 1.0, 0.0).astype(bf16)
    rank = jnp.dot(member, before, preferred_element_type=f32)
    slots = []
    for name in named:
        own_rank = jnp.sum(jnp.where(expert == name, rank, 0.0), axis=0, keepdims=True)
        step = ((name - column) & (NX - 1)).astype(f32)
        slots.append(jnp.where((name >> 2) == half, step * CAP + own_rank, -1.0))
    return slots


def hits_of(slots, count):
    slot = rows_iota(count).astype(f32)
    return [slot == own for own in slots]


def pack(slots, row_tile, outs, weights=None):
    hits = hits_of(slots, NX * CAP)
    chosen = jnp.where(hits[0] | hits[1], 1.0, 0.0).astype(bf16)
    if weights is not None:
        scale = jnp.where(hits[0], weights[0], 0.0) + jnp.where(hits[1], weights[1], 0.0)
        scale = ROUTE_SCALE * jnp.sum(scale, axis=1, keepdims=True)

    def tile(cols, carry):
        picked = jnp.dot(chosen, row_tile(cols), preferred_element_type=f32)
        if weights is not None:
            picked = scale * picked
        picked = picked.astype(bf16)
        for step in range(NX):
            outs[step][:, cols] = picked[step * CAP : (step + 1) * CAP]
        return carry

    each_tile(tile)


def prep_grad_body(aux_ref, rows_ref, *outs):
    aux = aux_ref[...]
    pack([aux[0:1], aux[1:2]], lambda cols: rows_ref[:, cols], outs, [aux[2:3], aux[3:4]])


def inverse_of(rows_ref):
    def tile(cols, total):
        values = rows_ref[:, cols].astype(f32)
        return total + jnp.sum(values * values, axis=1, keepdims=True)

    return lax.rsqrt(each_tile(tile, jnp.zeros((T, 1), f32)) / D + NORM_EPSILON)


def prep_norm_body(place_ref, ids_ref, rows_ref, gain_ref, router_ref, *refs):
    outs, aux_ref, normed_ref = refs[:NX], refs[NX], refs[NX + 1]
    named = [ids_ref[k : k + 1, :] for k in range(2)]
    slots = slots_of(named, place_ref)
    inverse = inverse_of(rows_ref)

    def tile(cols, carry):
        normed_ref[:, cols] = (rows_ref[:, cols].astype(f32) * inverse * gain_ref[:, cols]).astype(bf16)
        return carry

    each_tile(tile)
    pack(slots, lambda cols: normed_ref[:, cols], outs)
    logits = lax.dot_general(router_ref[...], normed_ref[...], NT, preferred_element_type=f32)
    scores = jax.nn.sigmoid(logits)
    expert = rows_iota(EXPERTS)
    picked = [jnp.sum(jnp.where(expert == name, scores, 0.0), axis=0, keepdims=True) for name in named]
    both = picked[0] + picked[1]
    lines = slots + [p / both for p in picked] + picked + [name.astype(f32) for name in named]
    for i, line in enumerate(lines):
        aux_ref[i : i + 1, :] = line


def fetch(copies):
    for copy in copies:
        copy.start()
    return copies


def finish(copies):
    for copy in copies:
        copy.wait()


def row_copies(pieces, rows_ref, sems):
    starts = [(i % NX * NZ + i // NX) * CAP for i in range(8)]
    return [
        pltpu.make_async_copy(piece, rows_ref.at[pl.ds(at, CAP), :], sems.at[i])
        for i, (piece, at) in enumerate(zip(pieces, starts))
    ]


def row_copy(source, target, sems, i):
    size = target.shape[1]
    rows = pl.ds(pl.multiple_of(i * size, size), size)
    return pltpu.make_async_copy(source.at[rows, :], target.at[i], sems.at[i])


def put_rows(outs, cols, rows):
    for step in range(NX):
        for z in range(NZ):
            at = (step * NZ + z) * CAP
            outs[z * NX + step][:, cols] = rows[at : at + CAP]


def strip_of(i):
    return pl.ds(pl.multiple_of(i * TF, TF), TF)


def lift_body(*refs):
    pieces, gate_ref, up_ref, a_ref, b_ref = refs[:8], refs[8], refs[9], refs[10], refs[11]
    rows_ref, gate, up, row_sems, gate_sem, up_sem = refs[12:]
    rows_in = fetch(row_copies(pieces, rows_ref, row_sems))
    gate_in = pltpu.make_async_copy(gate_ref, gate, gate_sem)
    up_in = pltpu.make_async_copy(up_ref, up, up_sem)
    gate_in.start()
    finish(rows_in)
    up_in.start()
    for weights, copy, out_ref in ((gate, gate_in, a_ref), (up, up_in, b_ref)):
        copy.wait()

        def strip(i, carry):
            out_ref[i] = jnp.dot(rows_ref[...], weights[:, strip_of(i)], preferred_element_type=f32)
            return carry

        lax.fori_loop(0, F // TF, strip, 0)


def back_body(*refs):
    pieces, down_ref, a_hbm, b_hbm, gate_ref, up_ref = refs[:8], refs[8], refs[9], refs[10], refs[11], refs[12]
    outs = refs[13:21]
    rows_ref, down, a_ref, b_ref, lifts, d_lift_ref, dot_ref = refs[21:28]
    row_sems, down_sems, a_sems, b_sems, gate_sems, up_sems = refs[28:]
    rows_in = fetch(row_copies(pieces, rows_ref, row_sems))

    def act_copies(i):
        return [
            row_copy(down_ref, down, down_sems, i),
            pltpu.make_async_copy(a_hbm.at[i], a_ref.at[i], a_sems.at[i]),
            pltpu.make_async_copy(b_hbm.at[i], b_ref.at[i], b_sems.at[i]),
        ]

    def back_copies(i):
        rows = pl.ds(pl.multiple_of(i * TB, TB), TB)
        return [
            pltpu.make_async_copy(gate_ref.at[rows, :], lifts.at[i, :, :F], gate_sems.at[i]),
            pltpu.make_async_copy(up_ref.at[rows, :], lifts.at[i, :, F:], up_sems.at[i]),
        ]

    for i in range(F // TF):
        fetch(act_copies(i))
    dot_ref[...] = jnp.zeros_like(dot_ref)
    finish(rows_in)

    def strip(i, carry):
        finish(act_copies(i))

        fetch(back_copies(i))
        d_act = lax.dot_general(rows_ref[...], down[i], NT, preferred_element_type=f32)
        a, b = a_ref[i], b_ref[i]
        s = jax.nn.sigmoid(a)
        both = (a * s * b).astype(bf16).astype(f32) * d_act
        dot_ref[...] += sum(both[:, n : n + 128] for n in range(0, TF, 128))
        d_lift_ref[:, strip_of(i)] = (d_act * b * s * (1.0 + a * (1.0 - s))).astype(bf16)
        d_lift_ref[:, pl.ds(pl.multiple_of(F + i * TF, TF), TF)] = (d_act * a * s).astype(bf16)
        return carry

    lax.fori_loop(0, F // TF, strip, 0)
    dots = jnp.sum(dot_ref[...], axis=1, keepdims=True)
    high = dots.astype(bf16).astype(f32)
    lane = lax.broadcasted_iota(jnp.int32, (ROWS, EXT), 1)
    extra = jnp.where(lane == 0, high, jnp.where(lane == 1, dots - high, 0.0)).astype(bf16)
    put_rows(outs, slice(D, D + EXT), extra)

    def tile(i, carry):
        finish(back_copies(i))
        back = lax.dot_general(d_lift_ref[...], lifts[i], NT, preferred_element_type=f32)
        put_rows(outs, pl.ds(pl.multiple_of(i * TB, TB), TB), back.astype(bf16))
        return carry

    lax.fori_loop(0, D // TB, tile, 0)


def forward_body(*refs):
    pieces, gate_ref, up_ref, down_ref = refs[:8], refs[8], refs[9], refs[10]
    outs = refs[11:19]
    rows_ref, gate, up, down, a_ref, active_ref, row_sems, gate_sem, up_sem, down_sem = refs[19:]
    rows_in = fetch(row_copies(pieces, rows_ref, row_sems))
    gate_in = pltpu.make_async_copy(gate_ref, gate, gate_sem)
    up_in = pltpu.make_async_copy(up_ref, up, up_sem)
    down_in = pltpu.make_async_copy(down_ref, down, down_sem)
    gate_in.start()
    finish(rows_in)
    up_in.start()
    gate_in.wait()
    down_in.start()

    def gate_strip(i, carry):
        a_ref[i] = jnp.dot(rows_ref[...], gate[:, strip_of(i)], preferred_element_type=f32)
        return carry

    lax.fori_loop(0, F // TF, gate_strip, 0)
    up_in.wait()

    def up_strip(i, carry):
        a = a_ref[i]
        b = jnp.dot(rows_ref[...], up[:, strip_of(i)], preferred_element_type=f32)
        active_ref[:, strip_of(i)] = (a * jax.nn.sigmoid(a) * b).astype(bf16)
        return carry

    lax.fori_loop(0, F // TF, up_strip, 0)
    down_in.wait()

    def tile(i, carry):
        cols = pl.ds(pl.multiple_of(i * TB, TB), TB)
        put_rows(outs, cols, jnp.dot(active_ref[...], down[:, cols], preferred_element_type=f32).astype(bf16))
        return carry

    lax.fori_loop(0, D // TB, tile, 0)


def split_weights(values):
    high = values.astype(bf16)
    return high, (values - high.astype(f32)).astype(bf16)


def stack_pieces(pieces, rows_ref):
    for step in range(NX):
        rows_ref[step * CAP : (step + 1) * CAP, :] = pieces[step][...]
    rows_ref[NX * CAP :, :] = jnp.zeros((256 - NX * CAP, rows_ref.shape[1]), bf16)


def mix_body(with_input, aux_ref, *refs):
    pieces, base_ref, out_ref, rows_ref = refs[:NX], refs[NX], refs[NX + 1], refs[NX + 2]
    stack_pieces(pieces, rows_ref)
    aux = aux_ref[...]
    hits = hits_of([aux[0:1], aux[1:2]], 256)
    weights = jnp.where(hits[0], aux[2:3], 0.0) + jnp.where(hits[1], aux[3:4], 0.0)
    high, low = split_weights(jnp.transpose(ROUTE_SCALE * weights))

    def tile(cols, carry):
        rows = rows_ref[:, cols]
        total = jnp.dot(high, rows, preferred_element_type=f32) + jnp.dot(low, rows, preferred_element_type=f32)
        if with_input:
            total = total + base_ref[:, cols].astype(f32)
        out_ref[:, cols] = total.astype(bf16)
        return carry

    each_tile(tile)


def grad_input_body(with_input, aux_ref, hidden_ref, gain_ref, router_ref, *refs):
    pieces, base_ref, out_ref, rows_ref, scaled_ref = refs[:NX], refs[NX], refs[NX + 1], refs[NX + 2], refs[NX + 3]
    stack_pieces(pieces, rows_ref)
    aux = aux_ref[...]
    hits = [jnp.where(hit, 1.0, 0.0) for hit in hits_of([aux[0:1], aux[1:2]], 256)]
    extra = jnp.transpose(rows_ref[:, D:].astype(f32))[:16].astype(bf16)
    pulls = []
    for hit in hits:
        found = jnp.dot(extra, hit.astype(bf16), preferred_element_type=f32)
        pulls.append(found[0:1] + found[1:2])
    route = router_ref[...]
    rows_ref[NX * CAP : NX * CAP + 16, :D] = jnp.concatenate([route, route], axis=0)
    slot = rows_iota(256)
    high = jnp.zeros((256, T), f32)
    low = jnp.zeros((256, T), f32)
    for k in range(2):
        weight, score, name = aux[2 + k : 3 + k], aux[4 + k : 5 + k], aux[6 + k : 7 + k].astype(jnp.int32)
        term = (pulls[k] - weight * (pulls[0] + pulls[1])) * (1.0 - score)
        first = term.astype(bf16).astype(f32)
        high = high + jnp.where(slot == name + NX * CAP, first, 0.0)
        low = low + jnp.where(slot == name + NX * CAP + EXPERTS, term - first, 0.0)
    mixing = jnp.transpose(hits[0] + hits[1] + high + low).astype(bf16)
    inverse = inverse_of(hidden_ref)

    def scale_tile(cols, against):
        scaled = jnp.dot(mixing, rows_ref[:, cols], preferred_element_type=f32) * gain_ref[:, cols]
        scaled_ref[:, cols] = scaled
        return against + jnp.sum(scaled * hidden_ref[:, cols].astype(f32), axis=1, keepdims=True)

    against = each_tile(scale_tile, jnp.zeros((T, 1), f32))
    pull = inverse * inverse * inverse * against / D

    def out_tile(cols, carry):
        out = inverse * scaled_ref[:, cols] - hidden_ref[:, cols].astype(f32) * pull
        if with_input:
            out = out + base_ref[:, cols].astype(f32)
        out_ref[:, cols] = out.astype(bf16)
        return carry

    each_tile(out_tile)


def ep_route(dz, dx):
    route = []
    for i in range(NZ * NX):
        z, x = divmod(i, NX)
        route.append((i, ((z + dz) % NZ) * NX + (x + dx) % NX))
    return route


def relay_route(sections, ds, dz):
    route = []
    for s in range(sections):
        for i in range(NZ * NX):
            z, x = divmod(i, NX)
            route.append((s * NZ * NX + i, ((s + ds) % sections) * NZ * NX + ((z + dz) % NZ) * NX + x))
    return route


def across(block):
    return lax.ppermute(block, "ep", ep_route(1, 0))


def spread(pieces):
    moved = list(pieces)
    for dx in (1, 3, 2):
        moved[dx] = lax.ppermute(pieces[dx], "ep", ep_route(0, dx))
    return moved


def collect(pieces):
    moved = list(pieces)
    for dx in (1, 3, 2):
        moved[dx] = lax.ppermute(pieces[dx], "ep", ep_route(0, -dx))
    return moved


def relay(block, ds, dz):
    return lax.ppermute(block, ("section", "ep"), relay_route(lax.axis_size("section"), ds, dz))


def step(
    fwd_input, bwd_input, bwd_grad, fwd_ids, bwd_ids, norm_gain, router, gate_w, up_w, down_w
):
    h_f, h_b, g = fwd_input[0], bwd_input[0], bwd_grad[0]
    gate, up, down = gate_w[0, 0], up_w[0, 0], down_w[0, 0]
    router_t = router[0].T
    ids_b, ids_f = bwd_ids[0].T, fwd_ids[0].T
    place = lax.axis_index("ep").astype(jnp.int32)[None]

    far_ids_b = across(ids_b)
    far_b = across(h_b)
    far_g = across(g)
    far_ids_f = across(ids_f)
    far_f = across(h_f)

    packed = [shape(CAP, D)] * NX
    aux_shape = shape(EXPERTS, T, dtype=f32)
    full = vspec((T, D))
    aux_spec = chip()
    piece_specs = [chip()] * NX
    pack_flops = 2 * NX * CAP * T * D

    def prep_grad(where, rows, aux, after=None):
        return call(
            prep_grad_body, packed, (aux, rows), grid=(1,), in_specs=[aux_spec, chip() if where == "far" else full], out_specs=piece_specs,
            flops=pack_flops, after=after,
        )

    def prep_norm(where, rows, ids, after=None):
        outs = call(
            prep_norm_body, packed + [aux_shape],
            (place, ids, rows, norm_gain, router_t), grid=(1,),
            in_specs=[sspec(), chip(), chip() if "far" in where else full, vspec((1, D)), vspec((EXPERTS, D))],
            out_specs=piece_specs + [aux_spec], scratch=[pltpu.VMEM((T, D), bf16)],
            flops=pack_flops, after=after,
        )
        return outs[:NX], outs[NX]

    packed_b, aux_b = prep_norm("b_own", h_b, ids_b)
    b_own = spread(packed_b)
    packed_g = prep_grad("own", g, aux_b)
    g_own = spread(packed_g)
    packed_bf, aux_b_far = prep_norm("b_far", far_b, far_ids_b, packed_g[0])
    b_far = spread(packed_bf)
    packed_f, aux_f = prep_norm("f_own", h_f, ids_f, packed_bf[0])
    packed_gf = prep_grad("far", far_g, aux_b_far, packed_f[0])
    g_far = spread(packed_gf)
    f_own = spread(packed_f)

    whole = pl.BlockSpec(memory_space=pl.ANY)
    rows_vmem = pltpu.VMEM((ROWS, D), bf16)
    lift_vmem, down_vmem = pltpu.VMEM((D, F), bf16), pltpu.VMEM((F, D), bf16)
    one = pltpu.SemaphoreType.DMA
    act_vmem = pltpu.VMEM((ROWS, F), bf16)
    act_f32_vmem = pltpu.VMEM((F // TF, ROWS, TF), f32)
    mat_flops = 2 * ROWS * D * F

    def sems(count):
        return pltpu.SemaphoreType.DMA((count,))

    def expert(body, outs, pieces, matrices, scratch, flops, after):
        return call(
            body, outs, (*pieces, *matrices), in_specs=[whole] * (8 + len(matrices)),
            out_specs=[chip()] * len(outs), scratch=scratch, flops=flops, after=after,
        )

    a, b = expert(
        lift_body, [shape(F // TF, ROWS, TF, dtype=f32)] * 2, (*b_own, *b_far), (gate, up),
        [rows_vmem, lift_vmem, lift_vmem, sems(8), one, one], 2 * mat_flops, packed_gf[0],
    )
    packed_ff, aux_f_far = prep_norm("f_far", far_f, far_ids_f, a)
    f_far = spread(packed_ff)
    returned = expert(
        back_body, [shape(CAP, D + EXT)] * 8, (*g_own, *g_far), (down, a, b, gate, up),
        [rows_vmem, pltpu.VMEM((F // TF, TF, D), bf16), act_f32_vmem, act_f32_vmem]
        + [pltpu.VMEM((D // TB, TB, 2 * F), bf16), pltpu.VMEM((ROWS, 2 * F), bf16), pltpu.VMEM((ROWS, 128), f32)]
        + [sems(8)] + [sems(F // TF)] * 3 + [sems(D // TB)] * 2, 3 * mat_flops, packed_ff[0],
    )
    back_far = collect(returned[NX:])
    back_own = collect(returned[:NX])
    outputs = expert(
        forward_body, [shape(CAP, D)] * 8, (*f_own, *f_far), (gate, up, down),
        [rows_vmem, lift_vmem, lift_vmem, down_vmem, act_f32_vmem, act_vmem, sems(8), one, one, one],
        3 * mat_flops, returned[0],
    )
    y_far = collect(outputs[NX:])
    y_own = collect(outputs[:NX])

    def mix(pieces, aux, base, with_input, after):
        return call(
            functools.partial(mix_body, with_input), [shape(T, D)], (aux, *pieces, base), grid=(1,),
            in_specs=[aux_spec] + piece_specs + [full if with_input else vspec((16, D))],
            out_specs=[full], scratch=[pltpu.VMEM((256, D), bf16)], flops=2 * pack_flops, after=after,
        )[0]

    def grad_input(pieces, aux, hidden, base, with_input, after):
        return call(
            functools.partial(grad_input_body, with_input), [shape(T, D)],
            (aux, hidden, norm_gain, router_t, *pieces, base), grid=(1,),
            in_specs=[aux_spec, full, vspec((1, D)), vspec((EXPERTS, D))] + piece_specs
            + [full if with_input else vspec((16, D))],
            out_specs=[full], scratch=[pltpu.VMEM((256, D + EXT), bf16), pltpu.VMEM((T, D), f32)],
            flops=2 * pack_flops, after=after,
        )[0]

    part_far = grad_input(back_far, aux_b_far, far_b, far_b, False, outputs[0])
    prev_far = relay(part_far, -1, 1)
    part_own = grad_input(back_own, aux_b, h_b, g, True, part_far)
    prev_own = relay(part_own, -1, 0)
    mix_far = mix(y_far, aux_f_far, far_f, False, part_own)
    next_far = relay(mix_far, 1, 1)
    mix_own = mix(y_own, aux_f, h_f, True, mix_far)
    next_own = relay(mix_own, 1, 0)

    def join(a, b):
        return (a.astype(f32) + b.astype(f32)).astype(bf16)

    return (join(next_own, next_far)[None], join(prev_own, prev_far)[None])


def solution(mesh):
    placed = (
        P("section", "ep", None),
        P("section", "ep", None),
        P("section", "ep", None),
        P("section", "ep", None),
        P("section", "ep", None),
        P("section", None),
        P("section", None, None),
        P("section", "ep", None, None),
        P("section", "ep", None, None),
        P("section", "ep", None, None),
    )
    return jax.shard_map(
        step,
        mesh=mesh,
        in_specs=placed,
        out_specs=(P("section", "ep", None), P("section", "ep", None)),
        check_vma=False,
    )
```

```python
import functools
import jax
import jax.numpy as jnp
from jax import lax
from jax.experimental import pallas as pl
from jax.experimental.pallas import tpu as pltpu
from jax.sharding import PartitionSpec as P


NORM_EPSILON = 1e-06
ROUTE_SCALE = 2.5

T = 128
D = 3584
F = 1024
CAP = 48
NX = 4
NZ = 2
EXPERTS = NX * NZ
ROWS = NX * NZ * CAP
TF = 512
TB = 1792
TD = 512
VMEM_LIMIT = 67043328
EXT = 128
f32 = jnp.float32
bf16 = jnp.bfloat16
NT = (((1,), (1,)), ((), ()))


def call(body, outs, ins, grid=None, in_specs=None, out_specs=None, scratch=(), flops=0, after=None):
    kwargs = {}
    if after is not None:
        inner, count = body, len(ins)
        ins = (*ins, after)
        in_specs = [*in_specs, pl.BlockSpec(memory_space=pl.ANY)]

        def body(*refs):
            inner(*refs[:count], *refs[count + 1 :])

    if grid is not None:
        kwargs["grid"] = grid
    if in_specs is not None:
        kwargs["in_specs"] = in_specs
    if out_specs is not None:
        kwargs["out_specs"] = out_specs
    moved = sum(a.size * a.dtype.itemsize for a in ins) + sum(o.size * o.dtype.itemsize for o in outs)
    return pl.pallas_call(
        body,
        out_shape=outs,
        scratch_shapes=list(scratch),
        cost_estimate=pl.CostEstimate(flops=int(flops), bytes_accessed=int(moved), transcendentals=0),
        compiler_params=pltpu.CompilerParams(vmem_limit_bytes=VMEM_LIMIT),
        **kwargs,
    )(*ins)


def vspec(shape, index=None):
    fixed = index if index is not None else (0,) * len(shape)
    return pl.BlockSpec(shape, lambda *_: fixed)


def chip():
    return pl.BlockSpec(memory_space=pltpu.VMEM)


def sspec():
    return pl.BlockSpec(memory_space=pltpu.SMEM)


def shape(*dims, dtype=bf16):
    return jax.ShapeDtypeStruct(dims, dtype)


def each_tile(body, start=0):
    carry = start
    for n in range(D // TD):
        carry = body(slice(n * TD, (n + 1) * TD), carry)
    return carry


def rows_iota(count):
    return lax.broadcasted_iota(jnp.int32, (count, T), 0)


def slots_of(named, place_ref):
    half, column = place_ref[0] >> 2, place_ref[0] & (NX - 1)
    expert = rows_iota(16)
    member = jnp.where((expert == named[0]) | (expert == named[1]), 1.0, 0.0).astype(bf16)
    before = jnp.where(rows_iota(T) < lax.broadcasted_iota(jnp.int32, (T, T), 1), 1.0, 0.0).astype(bf16)
    rank = jnp.dot(member, before, preferred_element_type=f32)
    slots = []
    for name in named:
        own_rank = jnp.sum(jnp.where(expert == name, rank, 0.0), axis=0, keepdims=True)
        step = ((name - column) & (NX - 1)).astype(f32)
        slots.append(jnp.where((name >> 2) == half, step * CAP + own_rank, -1.0))
    return slots


def hits_of(slots, count):
    slot = rows_iota(count).astype(f32)
    return [slot == own for own in slots]


def pack(slots, row_tile, outs, weights=None):
    hits = hits_of(slots, NX * CAP)
    chosen = jnp.where(hits[0] | hits[1], 1.0, 0.0).astype(bf16)
    if weights is not None:
        scale = jnp.where(hits[0], weights[0], 0.0) + jnp.where(hits[1], weights[1], 0.0)
        scale = ROUTE_SCALE * jnp.sum(scale, axis=1, keepdims=True)

    def tile(cols, carry):
        picked = jnp.dot(chosen, row_tile(cols), preferred_element_type=f32)
        if weights is not None:
            picked = scale * picked
        picked = picked.astype(bf16)
        for step in range(NX):
            outs[step][:, cols] = picked[step * CAP : (step + 1) * CAP]
        return carry

    each_tile(tile)


def prep_grad_body(aux_ref, rows_ref, *outs):
    aux = aux_ref[...]
    pack([aux[0:1], aux[1:2]], lambda cols: rows_ref[:, cols], outs, [aux[2:3], aux[3:4]])


def inverse_of(rows_ref):
    def tile(cols, total):
        values = rows_ref[:, cols].astype(f32)
        return total + jnp.sum(values * values, axis=1, keepdims=True)

    return lax.rsqrt(each_tile(tile, jnp.zeros((T, 1), f32)) / D + NORM_EPSILON)


def prep_norm_body(place_ref, ids_ref, rows_ref, gain_ref, router_ref, *refs):
    outs, aux_ref, normed_ref = refs[:NX], refs[NX], refs[NX + 1]
    named = [ids_ref[k : k + 1, :] for k in range(2)]
    slots = slots_of(named, place_ref)
    inverse = inverse_of(rows_ref)

    def tile(cols, carry):
        normed_ref[:, cols] = (rows_ref[:, cols].astype(f32) * inverse * gain_ref[:, cols]).astype(bf16)
        return carry

    each_tile(tile)
    pack(slots, lambda cols: normed_ref[:, cols], outs)
    logits = lax.dot_general(router_ref[...], normed_ref[...], NT, preferred_element_type=f32)
    scores = jax.nn.sigmoid(logits)
    expert = rows_iota(EXPERTS)
    picked = [jnp.sum(jnp.where(expert == name, scores, 0.0), axis=0, keepdims=True) for name in named]
    both = picked[0] + picked[1]
    lines = slots + [p / both for p in picked] + picked + [name.astype(f32) for name in named]
    for i, line in enumerate(lines):
        aux_ref[i : i + 1, :] = line


def fetch(copies):
    for copy in copies:
        copy.start()
    return copies


def finish(copies):
    for copy in copies:
        copy.wait()


def row_copies(pieces, rows_ref, sems):
    starts = [(i % NX * NZ + i // NX) * CAP for i in range(8)]
    return [
        pltpu.make_async_copy(piece, rows_ref.at[pl.ds(at, CAP), :], sems.at[i])
        for i, (piece, at) in enumerate(zip(pieces, starts))
    ]


def row_copy(source, target, sems, i):
    size = target.shape[1]
    rows = pl.ds(pl.multiple_of(i * size, size), size)
    return pltpu.make_async_copy(source.at[rows, :], target.at[i], sems.at[i])


def put_rows(outs, cols, rows):
    for step in range(NX):
        for z in range(NZ):
            at = (step * NZ + z) * CAP
            outs[z * NX + step][:, cols] = rows[at : at + CAP]


def strip_of(i):
    return pl.ds(pl.multiple_of(i * TF, TF), TF)


def lift_body(*refs):
    pieces, gate_ref, up_ref, a_ref, b_ref = refs[:8], refs[8], refs[9], refs[10], refs[11]
    rows_ref, gate, up, row_sems, gate_sem, up_sem = refs[12:]
    rows_in = fetch(row_copies(pieces, rows_ref, row_sems))
    gate_in = pltpu.make_async_copy(gate_ref, gate, gate_sem)
    up_in = pltpu.make_async_copy(up_ref, up, up_sem)
    gate_in.start()
    finish(rows_in)
    up_in.start()
    for weights, copy, out_ref in ((gate, gate_in, a_ref), (up, up_in, b_ref)):
        copy.wait()

        def strip(i, carry):
            out_ref[i] = jnp.dot(rows_ref[...], weights[:, strip_of(i)], preferred_element_type=f32)
            return carry

        lax.fori_loop(0, F // TF, strip, 0)


def back_body(*refs):
    pieces, down_ref, a_hbm, b_hbm, gate_ref, up_ref = refs[:8], refs[8], refs[9], refs[10], refs[11], refs[12]
    outs = refs[13:21]
    rows_ref, down, a_ref, b_ref, lifts, d_lift_ref, dot_ref = refs[21:28]
    row_sems, down_sems, a_sems, b_sems, gate_sems, up_sems = refs[28:]
    rows_in = fetch(row_copies(pieces, rows_ref, row_sems))

    def act_copies(i):
        return [
            row_copy(down_ref, down, down_sems, i),
            pltpu.make_async_copy(a_hbm.at[i], a_ref.at[i], a_sems.at[i]),
            pltpu.make_async_copy(b_hbm.at[i], b_ref.at[i], b_sems.at[i]),
        ]

    def back_copies(i):
        rows = pl.ds(pl.multiple_of(i * TB, TB), TB)
        return [
            pltpu.make_async_copy(gate_ref.at[rows, :], lifts.at[i, :, :F], gate_sems.at[i]),
            pltpu.make_async_copy(up_ref.at[rows, :], lifts.at[i, :, F:], up_sems.at[i]),
        ]

    for i in range(F // TF):
        fetch(act_copies(i))
    dot_ref[...] = jnp.zeros_like(dot_ref)
    finish(rows_in)

    def strip(i, carry):
        finish(act_copies(i))

        fetch(back_copies(i))
        d_act = lax.dot_general(rows_ref[...], down[i], NT, preferred_element_type=f32)
        a, b = a_ref[i], b_ref[i]
        s = jax.nn.sigmoid(a)
        both = (a * s * b).astype(bf16).astype(f32) * d_act
        dot_ref[...] += sum(both[:, n : n + 128] for n in range(0, TF, 128))
        d_lift_ref[:, strip_of(i)] = (d_act * b * s * (1.0 + a * (1.0 - s))).astype(bf16)
        d_lift_ref[:, pl.ds(pl.multiple_of(F + i * TF, TF), TF)] = (d_act * a * s).astype(bf16)
        return carry

    lax.fori_loop(0, F // TF, strip, 0)
    dots = jnp.sum(dot_ref[...], axis=1, keepdims=True)
    high = dots.astype(bf16).astype(f32)
    lane = lax.broadcasted_iota(jnp.int32, (ROWS, EXT), 1)
    extra = jnp.where(lane == 0, high, jnp.where(lane == 1, dots - high, 0.0)).astype(bf16)
    put_rows(outs, slice(D, D + EXT), extra)

    def tile(i, carry):
        finish(back_copies(i))
        back = lax.dot_general(d_lift_ref[...], lifts[i], NT, preferred_element_type=f32)
        put_rows(outs, pl.ds(pl.multiple_of(i * TB, TB), TB), back.astype(bf16))
        return carry

    lax.fori_loop(0, D // TB, tile, 0)


def forward_body(*refs):
    pieces, gate_ref, up_ref, down_ref = refs[:8], refs[8], refs[9], refs[10]
    outs = refs[11:27]
    rows_ref, gate, up, down, a_ref, active_ref, row_sems, gate_sem, up_sem, down_sem = refs[27:]
    rows_in = fetch(row_copies(pieces, rows_ref, row_sems))
    gate_in = pltpu.make_async_copy(gate_ref, gate, gate_sem)
    up_in = pltpu.make_async_copy(up_ref, up, up_sem)
    down_in = pltpu.make_async_copy(down_ref, down, down_sem)
    gate_in.start()
    finish(rows_in)
    up_in.start()
    gate_in.wait()
    down_in.start()

    def gate_strip(i, carry):
        a_ref[i] = jnp.dot(rows_ref[...], gate[:, strip_of(i)], preferred_element_type=f32)
        return carry

    lax.fori_loop(0, F // TF, gate_strip, 0)
    up_in.wait()

    def up_strip(i, carry):
        a = a_ref[i]
        b = jnp.dot(rows_ref[...], up[:, strip_of(i)], preferred_element_type=f32)
        active_ref[:, strip_of(i)] = (a * jax.nn.sigmoid(a) * b).astype(bf16)
        return carry

    lax.fori_loop(0, F // TF, up_strip, 0)
    down_in.wait()

    for i in range(D // TB):
        out = jnp.dot(active_ref[...], down[:, i * TB : (i + 1) * TB], preferred_element_type=f32).astype(bf16)
        put_rows(outs[i * 8 : (i + 1) * 8], slice(None), out)


def split_weights(values):
    high = values.astype(bf16)
    return high, (values - high.astype(f32)).astype(bf16)


def stack_pieces(pieces, rows_ref):
    for step in range(NX):
        rows_ref[step * CAP : (step + 1) * CAP, :] = pieces[step][...]
    rows_ref[NX * CAP :, :] = jnp.zeros((256 - NX * CAP, rows_ref.shape[1]), bf16)


def mix_body(with_input, aux_ref, *refs):
    pieces, base_ref, out_ref, rows_ref = refs[:NX], refs[NX], refs[NX + 1], refs[NX + 2]
    stack_pieces(pieces, rows_ref)
    aux = aux_ref[...]
    hits = hits_of([aux[0:1], aux[1:2]], 256)
    weights = jnp.where(hits[0], aux[2:3], 0.0) + jnp.where(hits[1], aux[3:4], 0.0)
    high, low = split_weights(jnp.transpose(ROUTE_SCALE * weights))
    rows = rows_ref[...]
    total = jnp.dot(high, rows, preferred_element_type=f32) + jnp.dot(low, rows, preferred_element_type=f32)
    if with_input:
        total = total + base_ref[...].astype(f32)
    out_ref[...] = total.astype(bf16)


def join_body(a_ref, b_ref, *refs):
    refs[-1][...] = (a_ref[...].astype(f32) + b_ref[...].astype(f32)).astype(bf16)


def join_last_body(a_ref, b_ref, _, c_ref, d_ref, out_ref, other_ref):
    join_body(a_ref, b_ref, out_ref)
    join_body(c_ref, d_ref, other_ref)


def grad_input_body(with_input, aux_ref, hidden_ref, gain_ref, router_ref, *refs):
    pieces, base_ref, out_ref, rows_ref, scaled_ref = refs[:NX], refs[NX], refs[NX + 1], refs[NX + 2], refs[NX + 3]
    stack_pieces(pieces, rows_ref)
    aux = aux_ref[...]
    hits = [jnp.where(hit, 1.0, 0.0) for hit in hits_of([aux[0:1], aux[1:2]], 256)]
    extra = jnp.transpose(rows_ref[:, D:].astype(f32))[:16].astype(bf16)
    pulls = []
    for hit in hits:
        found = jnp.dot(extra, hit.astype(bf16), preferred_element_type=f32)
        pulls.append(found[0:1] + found[1:2])
    route = router_ref[...]
    rows_ref[NX * CAP : NX * CAP + 16, :D] = jnp.concatenate([route, route], axis=0)
    slot = rows_iota(256)
    high = jnp.zeros((256, T), f32)
    low = jnp.zeros((256, T), f32)
    for k in range(2):
        weight, score, name = aux[2 + k : 3 + k], aux[4 + k : 5 + k], aux[6 + k : 7 + k].astype(jnp.int32)
        term = (pulls[k] - weight * (pulls[0] + pulls[1])) * (1.0 - score)
        first = term.astype(bf16).astype(f32)
        high = high + jnp.where(slot == name + NX * CAP, first, 0.0)
        low = low + jnp.where(slot == name + NX * CAP + EXPERTS, term - first, 0.0)
    mixing = jnp.transpose(hits[0] + hits[1] + high + low).astype(bf16)
    inverse = inverse_of(hidden_ref)

    def scale_tile(cols, against):
        scaled = jnp.dot(mixing, rows_ref[:, cols], preferred_element_type=f32) * gain_ref[:, cols]
        scaled_ref[:, cols] = scaled
        return against + jnp.sum(scaled * hidden_ref[:, cols].astype(f32), axis=1, keepdims=True)

    against = each_tile(scale_tile, jnp.zeros((T, 1), f32))
    pull = inverse * inverse * inverse * against / D

    def out_tile(cols, carry):
        out = inverse * scaled_ref[:, cols] - hidden_ref[:, cols].astype(f32) * pull
        if with_input:
            out = out + base_ref[:, cols].astype(f32)
        out_ref[:, cols] = out.astype(bf16)
        return carry

    each_tile(out_tile)


def ep_route(dz, dx):
    route = []
    for i in range(NZ * NX):
        z, x = divmod(i, NX)
        route.append((i, ((z + dz) % NZ) * NX + (x + dx) % NX))
    return route


def relay_route(sections, ds, dz):
    route = []
    for s in range(sections):
        for i in range(NZ * NX):
            z, x = divmod(i, NX)
            route.append((s * NZ * NX + i, ((s + ds) % sections) * NZ * NX + ((z + dz) % NZ) * NX + x))
    return route


def across(block):
    return lax.ppermute(block, "ep", ep_route(1, 0))


def spread(pieces):
    moved = list(pieces)
    for dx in (1, 3, 2):
        moved[dx] = lax.ppermute(pieces[dx], "ep", ep_route(0, dx))
    return moved


def collect(pieces):
    moved = list(pieces)
    for dx in (1, 3, 2):
        moved[dx] = lax.ppermute(pieces[dx], "ep", ep_route(0, -dx))
    return moved


def relay(block, ds, dz):
    return lax.ppermute(block, ("section", "ep"), relay_route(lax.axis_size("section"), ds, dz))


def step(
    fwd_input, bwd_input, bwd_grad, fwd_ids, bwd_ids, norm_gain, router, gate_w, up_w, down_w
):
    h_f, h_b, g = fwd_input[0], bwd_input[0], bwd_grad[0]
    gate, up, down = gate_w[0, 0], up_w[0, 0], down_w[0, 0]
    router_t = router[0].T
    ids_b, ids_f = bwd_ids[0].T, fwd_ids[0].T
    place = lax.axis_index("ep").astype(jnp.int32)[None]

    far_ids_b = across(ids_b)
    far_b = across(h_b)
    far_g = across(g)
    far_ids_f = across(ids_f)
    far_f = across(h_f)

    packed = [shape(CAP, D)] * NX
    aux_shape = shape(EXPERTS, T, dtype=f32)
    full = vspec((T, D))
    aux_spec = chip()
    piece_specs = [chip()] * NX
    pack_flops = 2 * NX * CAP * T * D

    def prep_grad(where, rows, aux, after=None):
        return call(
            prep_grad_body, packed, (aux, rows), grid=(1,), in_specs=[aux_spec, chip() if where == "far" else full], out_specs=piece_specs,
            flops=pack_flops, after=after,
        )

    def prep_norm(where, rows, ids, after=None):
        outs = call(
            prep_norm_body, packed + [aux_shape],
            (place, ids, rows, norm_gain, router_t), grid=(1,),
            in_specs=[sspec(), chip(), chip() if "far" in where else full, vspec((1, D)), vspec((EXPERTS, D))],
            out_specs=piece_specs + [aux_spec], scratch=[pltpu.VMEM((T, D), bf16)],
            flops=pack_flops, after=after,
        )
        return outs[:NX], outs[NX]

    packed_b, aux_b = prep_norm("b_own", h_b, ids_b)
    b_own = spread(packed_b)
    packed_g = prep_grad("own", g, aux_b)
    g_own = spread(packed_g)
    packed_bf, aux_b_far = prep_norm("b_far", far_b, far_ids_b, packed_g[0])
    b_far = spread(packed_bf)
    packed_f, aux_f = prep_norm("f_own", h_f, ids_f, packed_bf[0])
    packed_gf = prep_grad("far", far_g, aux_b_far, packed_f[0])
    g_far = spread(packed_gf)
    f_own = spread(packed_f)

    whole = pl.BlockSpec(memory_space=pl.ANY)
    rows_vmem = pltpu.VMEM((ROWS, D), bf16)
    lift_vmem, down_vmem = pltpu.VMEM((D, F), bf16), pltpu.VMEM((F, D), bf16)
    one = pltpu.SemaphoreType.DMA
    act_vmem = pltpu.VMEM((ROWS, F), bf16)
    act_f32_vmem = pltpu.VMEM((F // TF, ROWS, TF), f32)
    mat_flops = 2 * ROWS * D * F

    def sems(count):
        return pltpu.SemaphoreType.DMA((count,))

    def expert(body, outs, pieces, matrices, scratch, flops, after):
        return call(
            body, outs, (*pieces, *matrices), in_specs=[whole] * (8 + len(matrices)),
            out_specs=[chip()] * len(outs), scratch=scratch, flops=flops, after=after,
        )

    a, b = expert(
        lift_body, [shape(F // TF, ROWS, TF, dtype=f32)] * 2, (*b_own, *b_far), (gate, up),
        [rows_vmem, lift_vmem, lift_vmem, sems(8), one, one], 2 * mat_flops, packed_gf[0],
    )
    packed_ff, aux_f_far = prep_norm("f_far", far_f, far_ids_f, a)
    f_far = spread(packed_ff)
    returned = expert(
        back_body, [shape(CAP, D + EXT)] * 8, (*g_own, *g_far), (down, a, b, gate, up),
        [rows_vmem, pltpu.VMEM((F // TF, TF, D), bf16), act_f32_vmem, act_f32_vmem]
        + [pltpu.VMEM((D // TB, TB, 2 * F), bf16), pltpu.VMEM((ROWS, 2 * F), bf16), pltpu.VMEM((ROWS, 128), f32)]
        + [sems(8)] + [sems(F // TF)] * 3 + [sems(D // TB)] * 2, 3 * mat_flops, packed_ff[0],
    )
    back_far = collect(returned[NX:])
    back_own = collect(returned[:NX])
    outputs = expert(
        forward_body, [shape(CAP, TB)] * 16, (*f_own, *f_far), (gate, up, down),
        [rows_vmem, lift_vmem, lift_vmem, down_vmem, act_f32_vmem, act_vmem, sems(8), one, one, one],
        3 * mat_flops, returned[0],
    )

    def mix(where, i, pieces, aux, after):
        own = where == "own"
        return call(
            functools.partial(mix_body, own), [shape(T, TB)], (aux, *pieces, h_f if own else far_f), grid=(1,),
            in_specs=[aux_spec] + piece_specs + [vspec((T, TB), (0, i)) if own else vspec((16, TB))],
            out_specs=[vspec((T, TB))], scratch=[pltpu.VMEM((256, TB), bf16)], flops=pack_flops,
            after=after,
        )[0]

    def grad_input(pieces, aux, hidden, base, with_input, after):
        return call(
            functools.partial(grad_input_body, with_input), [shape(T, D)],
            (aux, hidden, norm_gain, router_t, *pieces, base), grid=(1,),
            in_specs=[aux_spec, full, vspec((1, D)), vspec((EXPERTS, D))] + piece_specs
            + [full if with_input else vspec((16, D))],
            out_specs=[full], scratch=[pltpu.VMEM((256, D + EXT), bf16), pltpu.VMEM((T, D), f32)],
            flops=2 * pack_flops, after=after,
        )[0]

    part_far = grad_input(back_far, aux_b_far, far_b, far_b, False, outputs[0])
    prev_far = relay(part_far, -1, 1)
    halves = range(D // TB)
    y_far = [collect(outputs[8 * i + NX : 8 * i + 8]) for i in halves]
    y_own = [collect(outputs[8 * i : 8 * i + NX]) for i in halves]
    last, next_far, next_own = part_far, [], []
    for i in halves:
        last = mix("far", i, y_far[i], aux_f_far, last)
        next_far.append(relay(last, 1, 1))
    last = part_own = grad_input(back_own, aux_b, h_b, g, True, last)
    prev_own = relay(part_own, -1, 0)
    for i in halves:
        last = mix("own", i, y_own[i], aux_f, last)
        next_own.append(relay(last, 1, 0))

    half = vspec((T, TB))

    def join(body, i, ins, in_specs, outs, out_specs, aliases):
        return pl.pallas_call(
            body, out_shape=[shape(T, D)] * outs, grid=(1,), in_specs=in_specs,
            out_specs=[vspec((T, TB), (0, i))] + out_specs, input_output_aliases=aliases,
            compiler_params=pltpu.CompilerParams(vmem_limit_bytes=VMEM_LIMIT),
        )(*ins)

    (first,) = join(join_body, 0, (next_own[0], next_far[0], last), [half, half, whole], 1, [], {})
    fwd_next, bwd_prev = join(
        join_last_body, 1, (next_own[1], next_far[1], first, prev_own, prev_far),
        [half, half, whole, full, full], 2, [full], {2: 0},
    )
    return (fwd_next[None], bwd_prev[None])


def solution(mesh):
    placed = (
        P("section", "ep", None),
        P("section", "ep", None),
        P("section", "ep", None),
        P("section", "ep", None),
        P("section", "ep", None),
        P("section", None),
        P("section", None, None),
        P("section", "ep", None, None),
        P("section", "ep", None, None),
        P("section", "ep", None, None),
    )
    return jax.shard_map(
        step,
        mesh=mesh,
        in_specs=placed,
        out_specs=(P("section", "ep", None), P("section", "ep", None)),
        check_vma=False,
    )
```

```python
import functools
import jax
import jax.numpy as jnp
from jax import lax
from jax.experimental import pallas as pl
from jax.experimental.pallas import tpu as pltpu
from jax.sharding import PartitionSpec as P


NORM_EPSILON = 1e-06
ROUTE_SCALE = 2.5

T = 128
D = 3584
F = 1024
CAP = 48
NX = 4
NZ = 2
EXPERTS = NX * NZ
ROWS = NX * NZ * CAP
TF = 512
TB = 1792
TD = 512
VMEM_LIMIT = 67043328
EXT = 128
f32 = jnp.float32
bf16 = jnp.bfloat16
NT = (((1,), (1,)), ((), ()))


def call(body, outs, ins, grid=None, in_specs=None, out_specs=None, scratch=(), flops=0, after=None):
    kwargs = {}
    if after is not None:
        inner, count = body, len(ins)
        ins = (*ins, after)
        in_specs = [*in_specs, pl.BlockSpec(memory_space=pl.ANY)]

        def body(*refs):
            inner(*refs[:count], *refs[count + 1 :])

    if grid is not None:
        kwargs["grid"] = grid
    if in_specs is not None:
        kwargs["in_specs"] = in_specs
    if out_specs is not None:
        kwargs["out_specs"] = out_specs
    moved = sum(a.size * a.dtype.itemsize for a in ins) + sum(o.size * o.dtype.itemsize for o in outs)
    return pl.pallas_call(
        body,
        out_shape=outs,
        scratch_shapes=list(scratch),
        cost_estimate=pl.CostEstimate(flops=int(flops), bytes_accessed=int(moved), transcendentals=0),
        compiler_params=pltpu.CompilerParams(vmem_limit_bytes=VMEM_LIMIT),
        **kwargs,
    )(*ins)


def vspec(shape, index=None):
    fixed = index if index is not None else (0,) * len(shape)
    return pl.BlockSpec(shape, lambda *_: fixed)


def chip():
    return pl.BlockSpec(memory_space=pltpu.VMEM)


def sspec():
    return pl.BlockSpec(memory_space=pltpu.SMEM)


def shape(*dims, dtype=bf16):
    return jax.ShapeDtypeStruct(dims, dtype)


def each_tile(body, start=0):
    carry = start
    for n in range(D // TD):
        carry = body(slice(n * TD, (n + 1) * TD), carry)
    return carry


def rows_iota(count):
    return lax.broadcasted_iota(jnp.int32, (count, T), 0)


def slots_of(named, place_ref):
    half, column = place_ref[0] >> 2, place_ref[0] & (NX - 1)
    expert = rows_iota(16)
    member = jnp.where((expert == named[0]) | (expert == named[1]), 1.0, 0.0).astype(bf16)
    before = jnp.where(rows_iota(T) < lax.broadcasted_iota(jnp.int32, (T, T), 1), 1.0, 0.0).astype(bf16)
    rank = jnp.dot(member, before, preferred_element_type=f32)
    slots = []
    for name in named:
        own_rank = jnp.sum(jnp.where(expert == name, rank, 0.0), axis=0, keepdims=True)
        step = ((name - column) & (NX - 1)).astype(f32)
        slots.append(jnp.where((name >> 2) == half, step * CAP + own_rank, -1.0))
    return slots


def hits_of(slots, count):
    slot = rows_iota(count).astype(f32)
    return [slot == own for own in slots]


def pack(slots, row_tile, outs, weights=None):
    hits = hits_of(slots, NX * CAP)
    chosen = jnp.where(hits[0] | hits[1], 1.0, 0.0).astype(bf16)
    if weights is not None:
        scale = jnp.where(hits[0], weights[0], 0.0) + jnp.where(hits[1], weights[1], 0.0)
        scale = ROUTE_SCALE * jnp.sum(scale, axis=1, keepdims=True)

    def tile(cols, carry):
        picked = jnp.dot(chosen, row_tile(cols), preferred_element_type=f32)
        if weights is not None:
            picked = scale * picked
        picked = picked.astype(bf16)
        for step in range(NX):
            outs[step][:, cols] = picked[step * CAP : (step + 1) * CAP]
        return carry

    each_tile(tile)


def prep_grad_body(aux_ref, rows_ref, *outs):
    aux = aux_ref[...]
    pack([aux[0:1], aux[1:2]], lambda cols: rows_ref[:, cols], outs, [aux[2:3], aux[3:4]])


def inverse_of(rows_ref):
    def tile(cols, total):
        values = rows_ref[:, cols].astype(f32)
        return total + jnp.sum(values * values, axis=1, keepdims=True)

    return lax.rsqrt(each_tile(tile, jnp.zeros((T, 1), f32)) / D + NORM_EPSILON)


def normalize(rows_ref, gain_ref, normed_ref):
    inverse = inverse_of(rows_ref)

    def tile(cols, carry):
        normed_ref[:, cols] = (rows_ref[:, cols].astype(f32) * inverse * gain_ref[:, cols]).astype(bf16)
        return carry

    each_tile(tile)


def route(named, slots, normed_ref, router_ref):
    logits = lax.dot_general(router_ref[...], normed_ref[...], NT, preferred_element_type=f32)
    scores = jax.nn.sigmoid(logits)
    expert = rows_iota(EXPERTS)
    picked = [jnp.sum(jnp.where(expert == name, scores, 0.0), axis=0, keepdims=True) for name in named]
    both = picked[0] + picked[1]
    return slots + [p / both for p in picked] + picked + [name.astype(f32) for name in named]


def prep_first_body(place_ref, ids_ref, rows_ref, gain_ref, *refs):
    outs, normed_ref = refs[:NX], refs[NX]
    slots = slots_of([ids_ref[k : k + 1, :] for k in range(2)], place_ref)
    normalize(rows_ref, gain_ref, normed_ref)
    pack(slots, lambda cols: normed_ref[:, cols], outs)


def prep_second_body(place_ref, ids_ref, rows_ref, gain_ref, router_ref, grad_ref, *refs):
    outs, aux_ref, normed_ref = refs[:NX], refs[NX], refs[NX + 1]
    named = [ids_ref[k : k + 1, :] for k in range(2)]
    slots = slots_of(named, place_ref)
    normalize(rows_ref, gain_ref, normed_ref)
    lines = route(named, slots, normed_ref, router_ref)
    for i, line in enumerate(lines):
        aux_ref[i : i + 1, :] = line
    pack(slots, lambda cols: grad_ref[:, cols], outs, lines[2:4])


def prep_norm_body(place_ref, ids_ref, rows_ref, gain_ref, router_ref, *refs):
    outs, aux_ref, normed_ref = refs[:NX], refs[NX], refs[NX + 1]
    named = [ids_ref[k : k + 1, :] for k in range(2)]
    slots = slots_of(named, place_ref)
    normalize(rows_ref, gain_ref, normed_ref)
    pack(slots, lambda cols: normed_ref[:, cols], outs)
    for i, line in enumerate(route(named, slots, normed_ref, router_ref)):
        aux_ref[i : i + 1, :] = line


def fetch(copies):
    for copy in copies:
        copy.start()
    return copies


def finish(copies):
    for copy in copies:
        copy.wait()


def row_copies(pieces, rows_ref, sems):
    starts = [(i % NX * NZ + i // NX) * CAP for i in range(8)]
    return [
        pltpu.make_async_copy(piece, rows_ref.at[pl.ds(at, CAP), :], sems.at[i])
        for i, (piece, at) in enumerate(zip(pieces, starts))
    ]


def row_copy(source, target, sems, i):
    size = target.shape[1]
    rows = pl.ds(pl.multiple_of(i * size, size), size)
    return pltpu.make_async_copy(source.at[rows, :], target.at[i], sems.at[i])


def put_rows(outs, cols, rows):
    for step in range(NX):
        for z in range(NZ):
            at = (step * NZ + z) * CAP
            outs[z * NX + step][:, cols] = rows[at : at + CAP]


def lift_copies(source, target, sems):
    halves = [pl.ds(i * TB, TB) for i in range(D // TB)]
    return [pltpu.make_async_copy(source.at[h, :], target.at[h, :], sems.at[i]) for i, h in enumerate(halves)]


def lift_strips(rows_ref, matrix, copies, out_ref):
    for n, copy in enumerate(copies):
        copy.wait()
        depth = slice(n * TB, (n + 1) * TB)

        def strip(i, carry):
            part = jnp.dot(rows_ref[:, depth], matrix[depth, strip_of(i)], preferred_element_type=f32)
            out_ref[i] = out_ref[i] + part if n else part
            return carry

        lax.fori_loop(0, F // TF, strip, 0)


def strip_of(i):
    return pl.ds(pl.multiple_of(i * TF, TF), TF)


def lift_body(*refs):
    pieces, gate_ref, up_ref, a_ref, b_ref = refs[:8], refs[8], refs[9], refs[10], refs[11]
    rows_ref, gate, up, row_sems, gate_sem, up_sem = refs[12:]
    rows_in = fetch(row_copies(pieces, rows_ref, row_sems))
    gate_in = fetch(lift_copies(gate_ref, gate, gate_sem))
    finish(rows_in)
    up_in = fetch(lift_copies(up_ref, up, up_sem))
    lift_strips(rows_ref, gate, gate_in, a_ref)
    lift_strips(rows_ref, up, up_in, b_ref)


def back_body(*refs):
    pieces, down_ref, a_hbm, b_hbm, gate_ref, up_ref = refs[:8], refs[8], refs[9], refs[10], refs[11], refs[12]
    outs = refs[13:21]
    rows_ref, down, a_ref, b_ref, lifts, d_lift_ref, dot_ref = refs[21:28]
    row_sems, down_sems, a_sems, b_sems, gate_sems, up_sems = refs[28:]
    rows_in = fetch(row_copies(pieces, rows_ref, row_sems))

    def act_copies(i):
        return [
            row_copy(down_ref, down, down_sems, i),
            pltpu.make_async_copy(a_hbm.at[i], a_ref.at[i], a_sems.at[i]),
            pltpu.make_async_copy(b_hbm.at[i], b_ref.at[i], b_sems.at[i]),
        ]

    def back_copies(i):
        rows = pl.ds(pl.multiple_of(i * TB, TB), TB)
        return [
            pltpu.make_async_copy(gate_ref.at[rows, :], lifts.at[i, :, :F], gate_sems.at[i]),
            pltpu.make_async_copy(up_ref.at[rows, :], lifts.at[i, :, F:], up_sems.at[i]),
        ]

    for i in range(F // TF):
        fetch(act_copies(i))
    dot_ref[...] = jnp.zeros_like(dot_ref)
    finish(rows_in)

    def strip(i, carry):
        finish(act_copies(i))

        fetch(back_copies(i))
        d_act = lax.dot_general(rows_ref[...], down[i], NT, preferred_element_type=f32)
        a, b = a_ref[i], b_ref[i]
        s = jax.nn.sigmoid(a)
        both = (a * s * b).astype(bf16).astype(f32) * d_act
        dot_ref[...] += sum(both[:, n : n + 128] for n in range(0, TF, 128))
        d_lift_ref[:, strip_of(i)] = (d_act * b * s * (1.0 + a * (1.0 - s))).astype(bf16)
        d_lift_ref[:, pl.ds(pl.multiple_of(F + i * TF, TF), TF)] = (d_act * a * s).astype(bf16)
        return carry

    lax.fori_loop(0, F // TF, strip, 0)
    dots = jnp.sum(dot_ref[...], axis=1, keepdims=True)
    high = dots.astype(bf16).astype(f32)
    lane = lax.broadcasted_iota(jnp.int32, (ROWS, EXT), 1)
    extra = jnp.where(lane == 0, high, jnp.where(lane == 1, dots - high, 0.0)).astype(bf16)
    put_rows(outs, slice(D, D + EXT), extra)

    def tile(i, carry):
        finish(back_copies(i))
        back = lax.dot_general(d_lift_ref[...], lifts[i], NT, preferred_element_type=f32)
        put_rows(outs, pl.ds(pl.multiple_of(i * TB, TB), TB), back.astype(bf16))
        return carry

    lax.fori_loop(0, D // TB, tile, 0)


def forward_body(*refs):
    pieces, gate_ref, up_ref, down_ref = refs[:8], refs[8], refs[9], refs[10]
    outs = refs[11:27]
    rows_ref, gate, up, down, a_ref, active_ref, row_sems, gate_sem, up_sem, down_sem = refs[27:]
    rows_in = fetch(row_copies(pieces, rows_ref, row_sems))
    gate_in = fetch(lift_copies(gate_ref, gate, gate_sem))
    up_in = pltpu.make_async_copy(up_ref, up, up_sem)
    down_in = pltpu.make_async_copy(down_ref, down, down_sem)
    finish(rows_in)
    up_in.start()
    down_in.start()
    lift_strips(rows_ref, gate, gate_in, a_ref)
    up_in.wait()

    def up_strip(i, carry):
        a = a_ref[i]
        b = jnp.dot(rows_ref[...], up[:, strip_of(i)], preferred_element_type=f32)
        active_ref[:, strip_of(i)] = (a * jax.nn.sigmoid(a) * b).astype(bf16)
        return carry

    lax.fori_loop(0, F // TF, up_strip, 0)
    down_in.wait()

    for i in range(D // TB):
        out = jnp.dot(active_ref[...], down[:, i * TB : (i + 1) * TB], preferred_element_type=f32).astype(bf16)
        put_rows(outs[i * 8 : (i + 1) * 8], slice(None), out)


def split_weights(values):
    high = values.astype(bf16)
    return high, (values - high.astype(f32)).astype(bf16)


def stack_pieces(pieces, rows_ref):
    for step in range(NX):
        rows_ref[step * CAP : (step + 1) * CAP, :] = pieces[step][...]
    rows_ref[NX * CAP :, :] = jnp.zeros((256 - NX * CAP, rows_ref.shape[1]), bf16)


def mix_body(with_input, aux_ref, *refs):
    pieces, base_ref, out_ref, rows_ref = refs[:NX], refs[NX], refs[NX + 1], refs[NX + 2]
    stack_pieces(pieces, rows_ref)
    aux = aux_ref[...]
    hits = hits_of([aux[0:1], aux[1:2]], 256)
    weights = jnp.where(hits[0], aux[2:3], 0.0) + jnp.where(hits[1], aux[3:4], 0.0)
    high, low = split_weights(jnp.transpose(ROUTE_SCALE * weights))
    rows = rows_ref[...]
    total = jnp.dot(high, rows, preferred_element_type=f32) + jnp.dot(low, rows, preferred_element_type=f32)
    if with_input:
        total = total + base_ref[...].astype(f32)
    out_ref[...] = total.astype(bf16)


def join_body(a_ref, b_ref, *refs):
    refs[-1][...] = (a_ref[...].astype(f32) + b_ref[...].astype(f32)).astype(bf16)


def grad_input_body(with_input, aux_ref, hidden_ref, gain_ref, router_ref, *refs):
    pieces, base_ref, out_ref, rows_ref, scaled_ref = refs[:NX], refs[NX], refs[NX + 1], refs[NX + 2], refs[NX + 3]
    stack_pieces(pieces, rows_ref)
    aux = aux_ref[...]
    hits = [jnp.where(hit, 1.0, 0.0) for hit in hits_of([aux[0:1], aux[1:2]], 256)]
    extra = jnp.transpose(rows_ref[:, D:].astype(f32))[:16].astype(bf16)
    pulls = []
    for hit in hits:
        found = jnp.dot(extra, hit.astype(bf16), preferred_element_type=f32)
        pulls.append(found[0:1] + found[1:2])
    router = router_ref[...]
    rows_ref[NX * CAP : NX * CAP + 16, :D] = jnp.concatenate([router, router], axis=0)
    slot = rows_iota(256)
    high = jnp.zeros((256, T), f32)
    low = jnp.zeros((256, T), f32)
    for k in range(2):
        weight, score, name = aux[2 + k : 3 + k], aux[4 + k : 5 + k], aux[6 + k : 7 + k].astype(jnp.int32)
        term = (pulls[k] - weight * (pulls[0] + pulls[1])) * (1.0 - score)
        first = term.astype(bf16).astype(f32)
        high = high + jnp.where(slot == name + NX * CAP, first, 0.0)
        low = low + jnp.where(slot == name + NX * CAP + EXPERTS, term - first, 0.0)
    mixing = jnp.transpose(hits[0] + hits[1] + high + low).astype(bf16)
    inverse = inverse_of(hidden_ref)

    def scale_tile(cols, against):
        scaled = jnp.dot(mixing, rows_ref[:, cols], preferred_element_type=f32) * gain_ref[:, cols]
        scaled_ref[:, cols] = scaled
        return against + jnp.sum(scaled * hidden_ref[:, cols].astype(f32), axis=1, keepdims=True)

    against = each_tile(scale_tile, jnp.zeros((T, 1), f32))
    pull = inverse * inverse * inverse * against / D

    def out_tile(cols, carry):
        out = inverse * scaled_ref[:, cols] - hidden_ref[:, cols].astype(f32) * pull
        if with_input:
            out = out + base_ref[:, cols].astype(f32)
        out_ref[:, cols] = out.astype(bf16)
        return carry

    each_tile(out_tile)


def ep_route(dz, dx):
    route = []
    for i in range(NZ * NX):
        z, x = divmod(i, NX)
        route.append((i, ((z + dz) % NZ) * NX + (x + dx) % NX))
    return route


def relay_route(sections, ds, dz):
    route = []
    for s in range(sections):
        for i in range(NZ * NX):
            z, x = divmod(i, NX)
            route.append((s * NZ * NX + i, ((s + ds) % sections) * NZ * NX + ((z + dz) % NZ) * NX + x))
    return route


def across(block):
    return lax.ppermute(block, "ep", ep_route(1, 0))


def spread(pieces):
    moved = list(pieces)
    for dx in (1, 3, 2):
        moved[dx] = lax.ppermute(pieces[dx], "ep", ep_route(0, dx))
    return moved


def collect(pieces):
    moved = list(pieces)
    for dx in (1, 3, 2):
        moved[dx] = lax.ppermute(pieces[dx], "ep", ep_route(0, -dx))
    return moved


def relay(block, ds, dz):
    return lax.ppermute(block, ("section", "ep"), relay_route(lax.axis_size("section"), ds, dz))


def step(
    fwd_input, bwd_input, bwd_grad, fwd_ids, bwd_ids, norm_gain, router, gate_w, up_w, down_w
):
    h_f, h_b, g = fwd_input[0], bwd_input[0], bwd_grad[0]
    gate, up, down = gate_w[0, 0], up_w[0, 0], down_w[0, 0]
    router_t = router[0].T
    ids_b, ids_f = bwd_ids[0].T, fwd_ids[0].T
    place = lax.axis_index("ep").astype(jnp.int32)[None]

    far_ids_b = across(ids_b)
    far_b = across(h_b)
    far_g = across(g)
    far_ids_f = across(ids_f)
    far_f = across(h_f)

    packed = [shape(CAP, D)] * NX
    aux_shape = shape(EXPERTS, T, dtype=f32)
    full = vspec((T, D))
    aux_spec = chip()
    piece_specs = [chip()] * NX
    pack_flops = 2 * NX * CAP * T * D

    def prep_grad(where, rows, aux, after=None):
        return call(
            prep_grad_body, packed, (aux, rows), grid=(1,), in_specs=[aux_spec, chip() if where == "far" else full], out_specs=piece_specs,
            flops=pack_flops, after=after,
        )

    def prep_norm(where, rows, ids, after=None):
        outs = call(
            prep_norm_body, packed + [aux_shape],
            (place, ids, rows, norm_gain, router_t), grid=(1,),
            in_specs=[sspec(), chip(), chip() if "far" in where else full, vspec((1, D)), vspec((EXPERTS, D))],
            out_specs=piece_specs + [aux_spec], scratch=[pltpu.VMEM((T, D), bf16)],
            flops=pack_flops, after=after,
        )
        return outs[:NX], outs[NX]

    packed_b = call(
        prep_first_body, packed, (place, ids_b, h_b, norm_gain), grid=(1,),
        in_specs=[sspec(), chip(), full, vspec((1, D))], out_specs=piece_specs, scratch=[pltpu.VMEM((T, D), bf16)],
        flops=pack_flops,
    )
    b_own = spread(packed_b)
    outs = call(
        prep_second_body, packed + [aux_shape], (place, ids_b, h_b, norm_gain, router_t, g), grid=(1,),
        in_specs=[sspec(), chip(), full, vspec((1, D)), vspec((EXPERTS, D)), full], out_specs=piece_specs + [aux_spec],
        scratch=[pltpu.VMEM((T, D), bf16)], flops=pack_flops, after=packed_b[0],
    )
    packed_g, aux_b = outs[:NX], outs[NX]
    g_own = spread(packed_g)
    packed_bf, aux_b_far = prep_norm("b_far", far_b, far_ids_b, packed_g[0])
    b_far = spread(packed_bf)
    packed_f, aux_f = prep_norm("f_own", h_f, ids_f, packed_bf[0])
    packed_gf = prep_grad("far", far_g, aux_b_far, packed_f[0])
    g_far = spread(packed_gf)
    f_own = spread(packed_f)

    whole = pl.BlockSpec(memory_space=pl.ANY)
    rows_vmem = pltpu.VMEM((ROWS, D), bf16)
    lift_vmem, down_vmem = pltpu.VMEM((D, F), bf16), pltpu.VMEM((F, D), bf16)
    one = pltpu.SemaphoreType.DMA
    act_vmem = pltpu.VMEM((ROWS, F), bf16)
    act_f32_vmem = pltpu.VMEM((F // TF, ROWS, TF), f32)
    mat_flops = 2 * ROWS * D * F

    def sems(count):
        return pltpu.SemaphoreType.DMA((count,))

    def expert(body, outs, pieces, matrices, scratch, flops, after):
        return call(
            body, outs, (*pieces, *matrices), in_specs=[whole] * (8 + len(matrices)),
            out_specs=[chip()] * len(outs), scratch=scratch, flops=flops, after=after,
        )

    a, b = expert(
        lift_body, [shape(F // TF, ROWS, TF, dtype=f32)] * 2, (*b_own, *b_far), (gate, up),
        [rows_vmem, lift_vmem, lift_vmem, sems(8), sems(2), sems(2)], 2 * mat_flops, packed_gf[0],
    )
    packed_ff, aux_f_far = prep_norm("f_far", far_f, far_ids_f, a)
    f_far = spread(packed_ff)
    returned = expert(
        back_body, [shape(CAP, D + EXT)] * 8, (*g_own, *g_far), (down, a, b, gate, up),
        [rows_vmem, pltpu.VMEM((F // TF, TF, D), bf16), act_f32_vmem, act_f32_vmem]
        + [pltpu.VMEM((D // TB, TB, 2 * F), bf16), pltpu.VMEM((ROWS, 2 * F), bf16), pltpu.VMEM((ROWS, 128), f32)]
        + [sems(8)] + [sems(F // TF)] * 3 + [sems(D // TB)] * 2, 3 * mat_flops, packed_ff[0],
    )
    back_far = collect(returned[NX:])
    back_own = collect(returned[:NX])
    outputs = expert(
        forward_body, [shape(CAP, TB)] * 16, (*f_own, *f_far), (gate, up, down),
        [rows_vmem, lift_vmem, lift_vmem, down_vmem, act_f32_vmem, act_vmem, sems(8), sems(2), one, one],
        3 * mat_flops, returned[0],
    )

    def mix(where, i, pieces, aux, after):
        own = where == "own"
        return call(
            functools.partial(mix_body, own), [shape(T, TB)], (aux, *pieces, h_f if own else far_f), grid=(1,),
            in_specs=[aux_spec] + piece_specs + [vspec((T, TB), (0, i)) if own else vspec((16, TB))],
            out_specs=[vspec((T, TB))], scratch=[pltpu.VMEM((256, TB), bf16)], flops=pack_flops,
            after=after,
        )[0]

    def grad_input(pieces, aux, hidden, base, with_input, after):
        return call(
            functools.partial(grad_input_body, with_input), [shape(T, D)],
            (aux, hidden, norm_gain, router_t, *pieces, base), grid=(1,),
            in_specs=[aux_spec, full, vspec((1, D)), vspec((EXPERTS, D))] + piece_specs
            + [full if with_input else vspec((16, D))],
            out_specs=[full], scratch=[pltpu.VMEM((256, D + EXT), bf16), pltpu.VMEM((T, D), f32)],
            flops=2 * pack_flops, after=after,
        )[0]

    part_far = grad_input(back_far, aux_b_far, far_b, far_b, False, outputs[0])
    prev_far = relay(part_far, -1, 1)
    halves = range(D // TB)
    y_far = [collect(outputs[8 * i + NX : 8 * i + 8]) for i in halves]
    y_own = [collect(outputs[8 * i : 8 * i + NX]) for i in halves]
    last, next_far, next_own = part_far, [], []
    for i in halves:
        last = mix("far", i, y_far[i], aux_f_far, last)
        next_far.append(relay(last, 1, 1))
    last = part_own = grad_input(back_own, aux_b, h_b, g, True, last)
    prev_own = relay(part_own, -1, 0)
    for i in halves:
        last = mix("own", i, y_own[i], aux_f, last)
        next_own.append(relay(last, 1, 0))

    half = vspec((T, TB))

    def join(body, i, ins, in_specs, outs, out_specs, aliases):
        return pl.pallas_call(
            body, out_shape=[shape(T, D)] * outs, grid=(1,), in_specs=in_specs,
            out_specs=[vspec((T, TB), (0, i))] + out_specs, input_output_aliases=aliases,
            compiler_params=pltpu.CompilerParams(vmem_limit_bytes=VMEM_LIMIT),
        )(*ins)

    (bwd_prev,) = call(
        join_body, [shape(T, D)], (prev_own, prev_far), grid=(1,), in_specs=[full, full], out_specs=[full],
        after=last,
    )
    (first,) = join(join_body, 0, (next_own[0], next_far[0], bwd_prev), [half, half, whole], 1, [], {})
    (fwd_next,) = join(join_body, 1, (next_own[1], next_far[1], first), [half, half, whole], 1, [], {2: 0})
    return (fwd_next[None], bwd_prev[None])


def solution(mesh):
    placed = (
        P("section", "ep", None),
        P("section", "ep", None),
        P("section", "ep", None),
        P("section", "ep", None),
        P("section", "ep", None),
        P("section", None),
        P("section", None, None),
        P("section", "ep", None, None),
        P("section", "ep", None, None),
        P("section", "ep", None, None),
    )
    return jax.shard_map(
        step,
        mesh=mesh,
        in_specs=placed,
        out_specs=(P("section", "ep", None), P("section", "ep", None)),
        check_vma=False,
    )
```

```python
import functools
import jax
import jax.numpy as jnp
from jax import lax
from jax.experimental import pallas as pl
from jax.experimental.pallas import tpu as pltpu
from jax.sharding import PartitionSpec as P


NORM_EPSILON = 1e-06
ROUTE_SCALE = 2.5

T = 128
D = 3584
F = 1024
CAP = 48
NX = 4
NZ = 2
EXPERTS = NX * NZ
ROWS = NX * NZ * CAP
TF = 512
TB = 1792
TD = 256
VMEM_LIMIT = 67043328
EXT = 128
f32 = jnp.float32
bf16 = jnp.bfloat16
NT = (((1,), (1,)), ((), ()))


def call(body, outs, ins, grid=None, in_specs=None, out_specs=None, scratch=(), flops=0, after=None):
    kwargs = {}
    if after is not None:
        inner, count = body, len(ins)
        ins = (*ins, after)
        in_specs = [*in_specs, pl.BlockSpec(memory_space=pl.ANY)]

        def body(*refs):
            inner(*refs[:count], *refs[count + 1 :])

    if grid is not None:
        kwargs["grid"] = grid
    if in_specs is not None:
        kwargs["in_specs"] = in_specs
    if out_specs is not None:
        kwargs["out_specs"] = out_specs
    moved = sum(a.size * a.dtype.itemsize for a in ins) + sum(o.size * o.dtype.itemsize for o in outs)
    return pl.pallas_call(
        body,
        out_shape=outs,
        scratch_shapes=list(scratch),
        cost_estimate=pl.CostEstimate(flops=int(flops), bytes_accessed=int(moved), transcendentals=0),
        compiler_params=pltpu.CompilerParams(vmem_limit_bytes=VMEM_LIMIT),
        **kwargs,
    )(*ins)


def vspec(shape, index=None):
    fixed = index if index is not None else (0,) * len(shape)
    return pl.BlockSpec(shape, lambda *_: fixed)


def chip():
    return pl.BlockSpec(memory_space=pltpu.VMEM)


def sspec():
    return pl.BlockSpec(memory_space=pltpu.SMEM)


def shape(*dims, dtype=bf16):
    return jax.ShapeDtypeStruct(dims, dtype)


def each_tile(body, start=0):
    carry = start
    for n in range(D // TD):
        carry = body(slice(n * TD, (n + 1) * TD), carry)
    return carry


def rows_iota(count):
    return lax.broadcasted_iota(jnp.int32, (count, T), 0)


def slots_of(named, place_ref):
    half, column = place_ref[0] >> 2, place_ref[0] & (NX - 1)
    expert = rows_iota(16)
    member = jnp.where((expert == named[0]) | (expert == named[1]), 1.0, 0.0).astype(bf16)
    before = jnp.where(rows_iota(T) < lax.broadcasted_iota(jnp.int32, (T, T), 1), 1.0, 0.0).astype(bf16)
    rank = jnp.dot(member, before, preferred_element_type=f32)
    slots = []
    for name in named:
        own_rank = jnp.sum(jnp.where(expert == name, rank, 0.0), axis=0, keepdims=True)
        step = ((name - column) & (NX - 1)).astype(f32)
        slots.append(jnp.where((name >> 2) == half, step * CAP + own_rank, -1.0))
    return slots


def hits_of(slots, count):
    slot = rows_iota(count).astype(f32)
    return [slot == own for own in slots]


def pack(slots, row_tile, outs, weights=None):
    hits = hits_of(slots, NX * CAP)
    chosen = jnp.where(hits[0] | hits[1], 1.0, 0.0).astype(bf16)
    if weights is not None:
        scale = jnp.where(hits[0], weights[0], 0.0) + jnp.where(hits[1], weights[1], 0.0)
        scale = ROUTE_SCALE * jnp.sum(scale, axis=1, keepdims=True)

    def tile(cols, carry):
        picked = jnp.dot(chosen, row_tile(cols), preferred_element_type=f32)
        if weights is not None:
            picked = scale * picked
        picked = picked.astype(bf16)
        for step in range(NX):
            outs[step][:, cols] = picked[step * CAP : (step + 1) * CAP]
        return carry

    each_tile(tile)


def prep_grad_body(aux_ref, rows_ref, *outs):
    aux = aux_ref[...]
    pack([aux[0:1], aux[1:2]], lambda cols: rows_ref[:, cols], outs, [aux[2:3], aux[3:4]])


def inverse_of(rows_ref):
    def tile(cols, total):
        values = rows_ref[:, cols].astype(f32)
        return total + jnp.sum(values * values, axis=1, keepdims=True)

    return lax.rsqrt(each_tile(tile, jnp.zeros((T, 1), f32)) / D + NORM_EPSILON)


def normalize(rows_ref, gain_ref, normed_ref):
    inverse = inverse_of(rows_ref)

    def tile(cols, carry):
        normed_ref[:, cols] = (rows_ref[:, cols].astype(f32) * inverse * gain_ref[:, cols]).astype(bf16)
        return carry

    each_tile(tile)


def route(named, slots, normed_ref, router_ref):
    logits = lax.dot_general(router_ref[...], normed_ref[...], NT, preferred_element_type=f32)
    scores = jax.nn.sigmoid(logits)
    expert = rows_iota(EXPERTS)
    picked = [jnp.sum(jnp.where(expert == name, scores, 0.0), axis=0, keepdims=True) for name in named]
    both = picked[0] + picked[1]
    return slots + [p / both for p in picked] + picked + [name.astype(f32) for name in named]


def prep_first_body(place_ref, ids_ref, rows_ref, gain_ref, *refs):
    outs, normed_ref = refs[:NX], refs[NX]
    slots = slots_of([ids_ref[k : k + 1, :] for k in range(2)], place_ref)
    normalize(rows_ref, gain_ref, normed_ref)
    pack(slots, lambda cols: normed_ref[:, cols], outs)


def prep_second_body(place_ref, ids_ref, rows_ref, gain_ref, router_ref, grad_ref, *refs):
    outs, aux_ref, normed_ref = refs[:NX], refs[NX], refs[NX + 1]
    named = [ids_ref[k : k + 1, :] for k in range(2)]
    slots = slots_of(named, place_ref)
    normalize(rows_ref, gain_ref, normed_ref)
    lines = route(named, slots, normed_ref, router_ref)
    for i, line in enumerate(lines):
        aux_ref[i : i + 1, :] = line
    pack(slots, lambda cols: grad_ref[:, cols], outs, lines[2:4])


def prep_norm_body(place_ref, ids_ref, rows_ref, gain_ref, router_ref, *refs):
    outs, aux_ref, normed_ref = refs[:NX], refs[NX], refs[NX + 1]
    named = [ids_ref[k : k + 1, :] for k in range(2)]
    slots = slots_of(named, place_ref)
    normalize(rows_ref, gain_ref, normed_ref)
    pack(slots, lambda cols: normed_ref[:, cols], outs)
    for i, line in enumerate(route(named, slots, normed_ref, router_ref)):
        aux_ref[i : i + 1, :] = line


def fetch(copies):
    for copy in copies:
        copy.start()
    return copies


def finish(copies):
    for copy in copies:
        copy.wait()


def row_copies(pieces, rows_ref, sems):
    starts = [(i % NX * NZ + i // NX) * CAP for i in range(8)]
    return [
        pltpu.make_async_copy(piece, rows_ref.at[pl.ds(at, CAP), :], sems.at[i])
        for i, (piece, at) in enumerate(zip(pieces, starts))
    ]


def row_copy(source, target, sems, i):
    size = target.shape[1]
    rows = pl.ds(pl.multiple_of(i * size, size), size)
    return pltpu.make_async_copy(source.at[rows, :], target.at[i], sems.at[i])


def put_rows(outs, cols, rows):
    for step in range(NX):
        for z in range(NZ):
            at = (step * NZ + z) * CAP
            outs[z * NX + step][:, cols] = rows[at : at + CAP]


def lift_copies(source, target, sems):
    halves = [pl.ds(i * TB, TB) for i in range(D // TB)]
    return [pltpu.make_async_copy(source.at[h, :], target.at[h, :], sems.at[i]) for i, h in enumerate(halves)]


def lift_strips(rows_ref, matrix, copies, out_ref):
    for n, copy in enumerate(copies):
        copy.wait()
        depth = slice(n * TB, (n + 1) * TB)

        def strip(i, carry):
            part = jnp.dot(rows_ref[:, depth], matrix[depth, strip_of(i)], preferred_element_type=f32)
            out_ref[i] = out_ref[i] + part if n else part
            return carry

        lax.fori_loop(0, F // TF, strip, 0)


def strip_of(i):
    return pl.ds(pl.multiple_of(i * TF, TF), TF)


def lift_body(*refs):
    pieces, gate_ref, up_ref, a_ref, b_ref = refs[:8], refs[8], refs[9], refs[10], refs[11]
    rows_ref, gate, up, row_sems, gate_sem, up_sem = refs[12:]
    rows_in = fetch(row_copies(pieces, rows_ref, row_sems))
    gate_in = fetch(lift_copies(gate_ref, gate, gate_sem))
    finish(rows_in)
    up_in = fetch(lift_copies(up_ref, up, up_sem))
    lift_strips(rows_ref, gate, gate_in, a_ref)
    lift_strips(rows_ref, up, up_in, b_ref)


def back_body(*refs):
    pieces, down_ref, a_hbm, b_hbm, gate_ref, up_ref = refs[:8], refs[8], refs[9], refs[10], refs[11], refs[12]
    outs = refs[13:21]
    rows_ref, down, a_ref, b_ref, lifts, d_lift_ref, dot_ref = refs[21:28]
    row_sems, down_sems, a_sems, b_sems, gate_sems, up_sems = refs[28:]
    rows_in = fetch(row_copies(pieces, rows_ref, row_sems))

    def act_copies(i):
        return [
            row_copy(down_ref, down, down_sems, i),
            pltpu.make_async_copy(a_hbm.at[i], a_ref.at[i], a_sems.at[i]),
            pltpu.make_async_copy(b_hbm.at[i], b_ref.at[i], b_sems.at[i]),
        ]

    def back_copies(i):
        rows = pl.ds(pl.multiple_of(i * TB, TB), TB)
        return [
            pltpu.make_async_copy(gate_ref.at[rows, :], lifts.at[i, :, :F], gate_sems.at[i]),
            pltpu.make_async_copy(up_ref.at[rows, :], lifts.at[i, :, F:], up_sems.at[i]),
        ]

    for i in range(F // TF):
        fetch(act_copies(i))
    dot_ref[...] = jnp.zeros_like(dot_ref)
    finish(rows_in)

    def strip(i, carry):
        finish(act_copies(i))

        fetch(back_copies(i))
        d_act = lax.dot_general(rows_ref[...], down[i], NT, preferred_element_type=f32)
        a, b = a_ref[i], b_ref[i]
        s = jax.nn.sigmoid(a)
        both = (a * s * b).astype(bf16).astype(f32) * d_act
        dot_ref[...] += sum(both[:, n : n + 128] for n in range(0, TF, 128))
        d_lift_ref[:, strip_of(i)] = (d_act * b * s * (1.0 + a * (1.0 - s))).astype(bf16)
        d_lift_ref[:, pl.ds(pl.multiple_of(F + i * TF, TF), TF)] = (d_act * a * s).astype(bf16)
        return carry

    lax.fori_loop(0, F // TF, strip, 0)
    dots = jnp.sum(dot_ref[...], axis=1, keepdims=True)
    high = dots.astype(bf16).astype(f32)
    lane = lax.broadcasted_iota(jnp.int32, (ROWS, EXT), 1)
    extra = jnp.where(lane == 0, high, jnp.where(lane == 1, dots - high, 0.0)).astype(bf16)
    put_rows(outs, slice(D, D + EXT), extra)

    def tile(i, carry):
        finish(back_copies(i))
        back = lax.dot_general(d_lift_ref[...], lifts[i], NT, preferred_element_type=f32)
        put_rows(outs, pl.ds(pl.multiple_of(i * TB, TB), TB), back.astype(bf16))
        return carry

    lax.fori_loop(0, D // TB, tile, 0)


def forward_body(*refs):
    pieces, gate_ref, up_ref, down_ref = refs[:8], refs[8], refs[9], refs[10]
    outs = refs[11:27]
    rows_ref, gate, up, down, a_ref, active_ref, row_sems, gate_sem, up_sem, down_sem = refs[27:]
    rows_in = fetch(row_copies(pieces, rows_ref, row_sems))
    gate_in = fetch(lift_copies(gate_ref, gate, gate_sem))
    up_in = pltpu.make_async_copy(up_ref, up, up_sem)
    down_in = pltpu.make_async_copy(down_ref, down, down_sem)
    finish(rows_in)
    up_in.start()
    down_in.start()
    lift_strips(rows_ref, gate, gate_in, a_ref)
    up_in.wait()

    def up_strip(i, carry):
        a = a_ref[i]
        b = jnp.dot(rows_ref[...], up[:, strip_of(i)], preferred_element_type=f32)
        active_ref[:, strip_of(i)] = (a * jax.nn.sigmoid(a) * b).astype(bf16)
        return carry

    lax.fori_loop(0, F // TF, up_strip, 0)
    down_in.wait()

    for i in range(D // TB):
        out = jnp.dot(active_ref[...], down[:, i * TB : (i + 1) * TB], preferred_element_type=f32).astype(bf16)
        put_rows(outs[i * 8 : (i + 1) * 8], slice(None), out)


def split_weights(values):
    high = values.astype(bf16)
    return high, (values - high.astype(f32)).astype(bf16)


def stack_pieces(pieces, rows_ref):
    for step in range(NX):
        rows_ref[step * CAP : (step + 1) * CAP, :] = pieces[step][...]
    rows_ref[NX * CAP :, :] = jnp.zeros((256 - NX * CAP, rows_ref.shape[1]), bf16)


def mix_body(with_input, aux_ref, *refs):
    pieces, base_ref, out_ref, rows_ref = refs[:NX], refs[NX], refs[NX + 1], refs[NX + 2]
    stack_pieces(pieces, rows_ref)
    aux = aux_ref[...]
    hits = hits_of([aux[0:1], aux[1:2]], 256)
    weights = jnp.where(hits[0], aux[2:3], 0.0) + jnp.where(hits[1], aux[3:4], 0.0)
    high, low = split_weights(jnp.transpose(ROUTE_SCALE * weights))
    rows = rows_ref[...]
    total = jnp.dot(high, rows, preferred_element_type=f32) + jnp.dot(low, rows, preferred_element_type=f32)
    if with_input:
        total = total + base_ref[...].astype(f32)
    out_ref[...] = total.astype(bf16)


def join_body(a_ref, b_ref, *refs):
    refs[-1][...] = (a_ref[...].astype(f32) + b_ref[...].astype(f32)).astype(bf16)


def grad_input_body(own, aux_ref, hidden_ref, gain_ref, *refs):
    pieces, refs = refs[:NX], refs[NX:]
    if own:
        router_ref, base_ref, far_pulls_ref, out_ref, rows_ref, scaled_ref = refs
    else:
        out_ref, pulls_ref, rows_ref, scaled_ref = refs
    stack_pieces(pieces, rows_ref)
    aux = aux_ref[...]
    hits = [jnp.where(hit, 1.0, 0.0) for hit in hits_of([aux[0:1], aux[1:2]], 256)]
    extra = jnp.transpose(rows_ref[:, D:].astype(f32))[:16].astype(bf16)
    pulls = []
    for hit in hits:
        found = jnp.dot(extra, hit.astype(bf16), preferred_element_type=f32)
        pulls.append(found[0:1] + found[1:2])
    mixing = hits[0] + hits[1]
    if own:
        pulls = [pulls[k] + far_pulls_ref[k : k + 1, :] for k in range(2)]
        rows_ref[NX * CAP : NX * CAP + 16, :D] = jnp.concatenate([router_ref[...]] * 2, axis=0)
        slot = rows_iota(256)
        for k in range(2):
            weight, score, name = aux[2 + k : 3 + k], aux[4 + k : 5 + k], aux[6 + k : 7 + k].astype(jnp.int32)
            d_logit = (pulls[k] - weight * (pulls[0] + pulls[1])) * (1.0 - score)
            mixing = mixing + jnp.where(slot == name + NX * CAP, d_logit, 0.0)
    else:
        for k in range(2):
            pulls_ref[k : k + 1, :] = pulls[k]
        pulls_ref[2:, :] = jnp.zeros((EXPERTS - 2, T), f32)
    mixing = jnp.transpose(mixing).astype(bf16)
    inverse = inverse_of(hidden_ref)

    def scale_tile(cols, against):
        scaled = jnp.dot(mixing, rows_ref[:, cols], preferred_element_type=f32) * gain_ref[:, cols]
        scaled_ref[:, cols] = scaled
        return against + jnp.sum(scaled * hidden_ref[:, cols].astype(f32), axis=1, keepdims=True)

    against = each_tile(scale_tile, jnp.zeros((T, 1), f32))
    pull = inverse * inverse * inverse * against / D

    def out_tile(cols, carry):
        out = inverse * scaled_ref[:, cols] - hidden_ref[:, cols].astype(f32) * pull
        if own:
            out = out + base_ref[:, cols].astype(f32)
        out_ref[:, cols] = out.astype(bf16)
        return carry

    each_tile(out_tile)


def ep_route(dz, dx):
    route = []
    for i in range(NZ * NX):
        z, x = divmod(i, NX)
        route.append((i, ((z + dz) % NZ) * NX + (x + dx) % NX))
    return route


def relay_route(sections, ds, dz):
    route = []
    for s in range(sections):
        for i in range(NZ * NX):
            z, x = divmod(i, NX)
            route.append((s * NZ * NX + i, ((s + ds) % sections) * NZ * NX + ((z + dz) % NZ) * NX + x))
    return route


def across(block):
    return lax.ppermute(block, "ep", ep_route(1, 0))


def spread(pieces):
    moved = list(pieces)
    for dx in (1, 3, 2):
        moved[dx] = lax.ppermute(pieces[dx], "ep", ep_route(0, dx))
    return moved


def collect(pieces):
    moved = list(pieces)
    for dx in (1, 3, 2):
        moved[dx] = lax.ppermute(pieces[dx], "ep", ep_route(0, -dx))
    return moved


def relay(block, ds, dz):
    return lax.ppermute(block, ("section", "ep"), relay_route(lax.axis_size("section"), ds, dz))


def step(
    fwd_input, bwd_input, bwd_grad, fwd_ids, bwd_ids, norm_gain, router, gate_w, up_w, down_w
):
    h_f, h_b, g = fwd_input[0], bwd_input[0], bwd_grad[0]
    gate, up, down = gate_w[0, 0], up_w[0, 0], down_w[0, 0]
    router_t = router[0].T
    ids_b, ids_f = bwd_ids[0].T, fwd_ids[0].T
    place = lax.axis_index("ep").astype(jnp.int32)[None]

    far_ids_b = across(ids_b)
    far_b = across(h_b)
    far_g = across(g)
    far_ids_f = across(ids_f)
    far_f = across(h_f)

    packed = [shape(CAP, D)] * NX
    aux_shape = shape(EXPERTS, T, dtype=f32)
    full = vspec((T, D))
    aux_spec = chip()
    piece_specs = [chip()] * NX
    pack_flops = 2 * NX * CAP * T * D

    def prep_grad(where, rows, aux, after=None):
        return call(
            prep_grad_body, packed, (aux, rows), grid=(1,), in_specs=[aux_spec, chip() if where == "far" else full], out_specs=piece_specs,
            flops=pack_flops, after=after,
        )

    def prep_norm(where, rows, ids, after=None):
        outs = call(
            prep_norm_body, packed + [aux_shape],
            (place, ids, rows, norm_gain, router_t), grid=(1,),
            in_specs=[sspec(), chip(), chip() if "far" in where else full, vspec((1, D)), vspec((EXPERTS, D))],
            out_specs=piece_specs + [aux_spec], scratch=[pltpu.VMEM((T, D), bf16)],
            flops=pack_flops, after=after,
        )
        return outs[:NX], outs[NX]

    packed_b = call(
        prep_first_body, packed, (place, ids_b, h_b, norm_gain), grid=(1,),
        in_specs=[sspec(), chip(), full, vspec((1, D))], out_specs=piece_specs, scratch=[pltpu.VMEM((T, D), bf16)],
        flops=pack_flops,
    )
    b_own = spread(packed_b)
    outs = call(
        prep_second_body, packed + [aux_shape], (place, ids_b, h_b, norm_gain, router_t, g), grid=(1,),
        in_specs=[sspec(), chip(), full, vspec((1, D)), vspec((EXPERTS, D)), full], out_specs=piece_specs + [aux_spec],
        scratch=[pltpu.VMEM((T, D), bf16)], flops=pack_flops, after=packed_b[0],
    )
    packed_g, aux_b = outs[:NX], outs[NX]
    g_own = spread(packed_g)
    packed_bf, aux_b_far = prep_norm("b_far", far_b, far_ids_b, packed_g[0])
    b_far = spread(packed_bf)
    packed_f, aux_f = prep_norm("f_own", h_f, ids_f, packed_bf[0])
    packed_gf = prep_grad("far", far_g, aux_b_far, packed_f[0])
    g_far = spread(packed_gf)
    f_own = spread(packed_f)

    whole = pl.BlockSpec(memory_space=pl.ANY)
    rows_vmem = pltpu.VMEM((ROWS, D), bf16)
    lift_vmem, down_vmem = pltpu.VMEM((D, F), bf16), pltpu.VMEM((F, D), bf16)
    one = pltpu.SemaphoreType.DMA
    act_vmem = pltpu.VMEM((ROWS, F), bf16)
    act_f32_vmem = pltpu.VMEM((F // TF, ROWS, TF), f32)
    mat_flops = 2 * ROWS * D * F

    def sems(count):
        return pltpu.SemaphoreType.DMA((count,))

    def expert(body, outs, pieces, matrices, scratch, flops, after):
        return call(
            body, outs, (*pieces, *matrices), in_specs=[whole] * (8 + len(matrices)),
            out_specs=[chip()] * len(outs), scratch=scratch, flops=flops, after=after,
        )

    a, b = expert(
        lift_body, [shape(F // TF, ROWS, TF, dtype=f32)] * 2, (*b_own, *b_far), (gate, up),
        [rows_vmem, lift_vmem, lift_vmem, sems(8), sems(2), sems(2)], 2 * mat_flops, packed_gf[0],
    )
    packed_ff, aux_f_far = prep_norm("f_far", far_f, far_ids_f, a)
    f_far = spread(packed_ff)
    returned = expert(
        back_body, [shape(CAP, D + EXT)] * 8, (*g_own, *g_far), (down, a, b, gate, up),
        [rows_vmem, pltpu.VMEM((F // TF, TF, D), bf16), act_f32_vmem, act_f32_vmem]
        + [pltpu.VMEM((D // TB, TB, 2 * F), bf16), pltpu.VMEM((ROWS, 2 * F), bf16), pltpu.VMEM((ROWS, 128), f32)]
        + [sems(8)] + [sems(F // TF)] * 3 + [sems(D // TB)] * 2, 3 * mat_flops, packed_ff[0],
    )
    back_far = collect(returned[NX:])
    back_own = collect(returned[:NX])
    outputs = expert(
        forward_body, [shape(CAP, TB)] * 16, (*f_own, *f_far), (gate, up, down),
        [rows_vmem, lift_vmem, lift_vmem, down_vmem, act_f32_vmem, act_vmem, sems(8), sems(2), one, one],
        3 * mat_flops, returned[0],
    )

    def mix(where, i, pieces, aux, after):
        own = where == "own"
        return call(
            functools.partial(mix_body, own), [shape(T, TB)], (aux, *pieces, h_f if own else far_f), grid=(1,),
            in_specs=[aux_spec] + piece_specs + [vspec((T, TB), (0, i)) if own else vspec((16, TB))],
            out_specs=[vspec((T, TB))], scratch=[pltpu.VMEM((256, TB), bf16)], flops=pack_flops,
            after=after,
        )[0]

    def grad_input(pieces, aux, hidden, more, outs, after):
        own = len(more) > 0
        return call(
            functools.partial(grad_input_body, own), outs, (aux, hidden, norm_gain, *pieces, *more), grid=(1,),
            in_specs=[aux_spec, full, vspec((1, D))] + piece_specs + ([vspec((EXPERTS, D)), full, aux_spec] if own else []),
            out_specs=[full, aux_spec][: len(outs)], scratch=[pltpu.VMEM((256, D + EXT), bf16), pltpu.VMEM((T, D), f32)],
            flops=2 * pack_flops, after=after,
        )

    part_far, pulls = grad_input(back_far, aux_b_far, far_b, (), [shape(T, D), aux_shape], outputs[0])
    prev_far = relay(part_far, -1, 1)
    far_pulls = across(pulls)
    halves = range(D // TB)
    y_far = [collect(outputs[8 * i + NX : 8 * i + 8]) for i in halves]
    y_own = [collect(outputs[8 * i : 8 * i + NX]) for i in halves]
    last, next_far, next_own = part_far, [], []
    for i in halves:
        last = mix("far", i, y_far[i], aux_f_far, last)
        next_far.append(relay(last, 1, 1))
    (last,) = (part_own,) = grad_input(back_own, aux_b, h_b, (router_t, g, far_pulls), [shape(T, D)], last)
    prev_own = relay(part_own, -1, 0)
    for i in halves:
        last = mix("own", i, y_own[i], aux_f, last)
        next_own.append(relay(last, 1, 0))

    half = vspec((T, TB))

    def join(body, i, ins, in_specs, outs, out_specs, aliases):
        return pl.pallas_call(
            body, out_shape=[shape(T, D)] * outs, grid=(1,), in_specs=in_specs,
            out_specs=[vspec((T, TB), (0, i))] + out_specs, input_output_aliases=aliases,
            compiler_params=pltpu.CompilerParams(vmem_limit_bytes=VMEM_LIMIT),
        )(*ins)

    (bwd_prev,) = call(
        join_body, [shape(T, D)], (prev_own, prev_far), grid=(1,), in_specs=[full, full], out_specs=[full],
        after=last,
    )
    (first,) = join(join_body, 0, (next_own[0], next_far[0], bwd_prev), [half, half, whole], 1, [], {})
    (fwd_next,) = join(join_body, 1, (next_own[1], next_far[1], first), [half, half, whole], 1, [], {2: 0})
    return (fwd_next[None], bwd_prev[None])


def solution(mesh):
    placed = (
        P("section", "ep", None),
        P("section", "ep", None),
        P("section", "ep", None),
        P("section", "ep", None),
        P("section", "ep", None),
        P("section", None),
        P("section", None, None),
        P("section", "ep", None, None),
        P("section", "ep", None, None),
        P("section", "ep", None, None),
    )
    return jax.shard_map(
        step,
        mesh=mesh,
        in_specs=placed,
        out_specs=(P("section", "ep", None), P("section", "ep", None)),
        check_vma=False,
    )
```
